8 devices in a mesh: batch: 1 (over z), z: 2 (over y), y: 2 (over x), x: 2 (over core).
Axes of the slice: x: 2, y: 2, z: 1, core: 2. Of those that a mesh axis runs over, the one named last changes fastest.
Arguments:
- source: float32 [256, 256, 256], P(('batch', 'z'), 'y', 'x')
- initial_guess: float32 [256, 256, 256], P(('batch', 'z'), 'y', 'x')
Outputs:
- output: float32 [256, 256, 256], P(('batch', 'z'), 'y', 'x')
All inputs are finite; a program needn't handle non-finite values.
Results may differ from the reference program's by a relative error of at most 0.001.
Values sent between devices are 32-bit elements.
A program may use at most 1 GiB of HBM per device.

```python
import math
import jax
import jax.numpy as jnp
from jax import lax

N = 256
CYCLES = 2
PRE = 2
POST = 2
COARSE_SWEEPS = 24


def level_count(fine_edge):
    count = 0
    edge_now = fine_edge
    for step_index in range(16):
        if edge_now % 2 == 0 and edge_now // 2 >= 4:
            edge_now = edge_now // 2
            count = count + 1
    return count


LEVELS = level_count(N)


def sine_table(modes, edge):
    centres = (jnp.arange(edge, dtype=jnp.float32) + 0.5) / edge
    waves = jnp.arange(1, modes + 1, dtype=jnp.float32)
    return jnp.sin(math.pi * waves[:, None] * centres[None, :])


def mode_field(coeffs, table):
    stage = jnp.einsum('abc,ck->abk', coeffs, table)
    stage = jnp.einsum('abk,bj->ajk', stage, table)
    return jnp.einsum('ajk,ai->ijk', stage, table)


def setup_inputs(seed: int = 0, part: int = 0) -> dict:
    base_key = jax.random.fold_in(jax.random.key(seed), part)
    key_sol, key_noise, key_init, key_rough = jax.random.split(base_key, 4)
    waves = jnp.arange(1, 9, dtype=jnp.float32)
    wave_sq = waves[:, None, None] ** 2 + waves[None, :, None] ** 2 + waves[None, None, :] ** 2
    pi_sq = math.pi * math.pi
    sol_coeffs = 2.0 * jax.random.normal(key_sol, (8, 8, 8), jnp.float32) / jnp.sqrt(wave_sq)
    table = sine_table(8, N)
    smooth_source = mode_field(pi_sq * sol_coeffs * wave_sq, table)
    rough_source = 2.0 * N * N * jax.random.normal(key_noise, (N, N, N), jnp.float32)
    init_coeffs = 3.5 * jax.random.normal(key_init, (4, 4, 4), jnp.float32)
    smooth_guess = mode_field(init_coeffs, table[:4])
    rough_guess = jax.random.normal(key_rough, (N, N, N), jnp.float32)
    return {'source': smooth_source + rough_source, 'initial_guess': smooth_guess + rough_guess}


def shifted(grid, axis):
    extent = grid.shape[axis]
    first = lax.slice_in_dim(grid, 0, 1, axis=axis)
    last = lax.slice_in_dim(grid, extent - 1, extent, axis=axis)
    below = jnp.concatenate([-first, lax.slice_in_dim(grid, 0, extent - 1, axis=axis)], axis=axis)
    above = jnp.concatenate([lax.slice_in_dim(grid, 1, extent, axis=axis), -last], axis=axis)
    return below, above


def neighbour_sum(grid):
    total = jnp.zeros_like(grid)
    for axis in range(3):
        below, above = shifted(grid, axis)
        total = total + below + above
    return total


def red_mask(edge):
    coords = jnp.arange(edge)
    return (coords[:, None, None] + coords[None, :, None] + coords[None, None, :]) % 2 == 0


def gs_sweep(iterate, source, step_sq, red_cells):
    scaled = step_sq * source
    updated = (scaled + neighbour_sum(iterate)) / 6.0
    iterate = jnp.where(red_cells, updated, iterate)
    updated = (scaled + neighbour_sum(iterate)) / 6.0
    return jnp.where(red_cells, iterate, updated)


def residual(iterate, source, step_sq):
    return source - (6.0 * iterate - neighbour_sum(iterate)) / step_sq


def restrict(grid):
    grid_shape = grid.shape
    folded = grid.reshape(grid_shape[0] // 2, 2, grid_shape[1] // 2, 2, grid_shape[2] // 2, 2)
    return folded.mean(axis=(1, 3, 5))


def prolong(coarse):
    fine = coarse
    for axis in range(3):
        below, above = shifted(fine, axis)
        even_cells = 0.75 * fine + 0.25 * below
        odd_cells = 0.75 * fine + 0.25 * above
        new_shape = list(fine.shape)
        new_shape[axis] = 2 * new_shape[axis]
        fine = jnp.stack([even_cells, odd_cells], axis=axis + 1).reshape(new_shape)
    return fine


def vcycle(iterate, source, level):
    step_sq = (1.0 / (N >> level)) ** 2
    red_cells = red_mask(N >> level)
    if level == LEVELS:
        return lax.fori_loop(0, COARSE_SWEEPS, lambda sweep_index, current: gs_sweep(current, source, step_sq, red_cells), iterate)
    for sweep_index in range(PRE):
        iterate = gs_sweep(iterate, source, step_sq, red_cells)
    coarse_source = restrict(residual(iterate, source, step_sq))
    correction = vcycle(jnp.zeros_like(coarse_source), coarse_source, level + 1)
    iterate = iterate + prolong(correction)
    for sweep_index in range(POST):
        iterate = gs_sweep(iterate, source, step_sq, red_cells)
    return iterate


def reference(source, initial_guess):
    iterate = initial_guess
    for cycle_index in range(CYCLES):
        iterate = vcycle(iterate, source, 0)
    return iterate
```

```python
import functools

import jax
import jax.numpy as jnp
from jax import lax
from jax.experimental import pallas as pl
from jax.experimental.pallas import tpu as pltpu
from jax.sharding import PartitionSpec as P

CYCLES = 2
COARSE_SWEEPS = 24
LANES = 128
TILE = 8
MESH = pl.DeviceIdType.MESH
F32 = jnp.float32
SIXTH = 1.0 / 6.0
RED, BLACK = 0, 1
HIGHEST = lax.Precision.HIGHEST


def mult8(value):
    return value if isinstance(value, int) else pl.multiple_of(value, TILE)


def rows(start, size):
    return pl.ds(mult8(start), size)


class Level:
    def __init__(self, n, dist, width, unroll):
        self.n = n
        self.planes = n // 2
        self.nb = max(n, TILE)
        self.pitch = self.nb + 16
        self.dist = dist
        self.width = min(width, self.nb)
        self.chunks = self.nb // self.width
        self.unroll = min(unroll, self.planes)

    def scratch(self):
        cells = pltpu.VMEM(((self.planes + 2) * self.pitch, LANES), F32)
        packed = pltpu.VMEM((self.planes * self.nb, LANES), F32)
        shapes = dict(v0=cells, v1=cells, g0=packed, g1=packed)
        if self.dist:
            face_x = pltpu.VMEM((self.nb, LANES), F32)
            face_y = pltpu.VMEM((self.planes, LANES), F32)
            for colour in (RED, BLACK):
                shapes[f'fx{colour}'] = face_x
                shapes[f'hx{colour}'] = face_x
                shapes[f'fy{colour}'] = face_y
                shapes[f'hy{colour}'] = face_y
            for axis in ('x', 'z'):
                shapes[f's{axis}'] = pltpu.SemaphoreType.DMA((2 * self.chunks,))
                shapes[f'r{axis}'] = pltpu.SemaphoreType.DMA((2 * self.chunks,))
            shapes['sy'] = pltpu.SemaphoreType.DMA((2,))
            shapes['ry'] = pltpu.SemaphoreType.DMA((2,))
        return shapes

    def bind(self, refs):
        self.v = (refs['v0'], refs['v1'])
        self.g = (refs['g0'], refs['g1'])
        if self.dist:
            self.fx = (refs['fx0'], refs['fx1'])
            self.hx = (refs['hx0'], refs['hx1'])
            self.fy = (refs['fy0'], refs['fy1'])
            self.hy = (refs['hy0'], refs['hy1'])
            self.sems = {key: refs[key] for key in ('sx', 'rx', 'sz', 'rz', 'sy', 'ry')}


def make_levels(edge):
    levels = [Level(edge, True, 32, 4), Level(edge // 2, True, 32, 4)]
    n = edge // 2
    while n >= 4:
        levels.append(Level(n, False, 32, 4))
        n = n // 2
    return levels


def kernel_body(names, edge, *args):
    refs = dict(zip(names, args))
    xi, yi, zi = lax.axis_index('x'), lax.axis_index('y'), lax.axis_index('z')
    levels = make_levels(edge)
    for index, level in enumerate(levels):
        prefix = f'L{index}_'
        level.bind({key[len(prefix):]: ref for key, ref in refs.items() if key.startswith(prefix)})

    def lanes(size):
        return lax.broadcasted_iota(jnp.int32, (size, LANES), 1)

    def even_mask(size):
        return lax.rem(lanes(size) + lax.broadcasted_iota(jnp.int32, (size, LANES), 0), 2) == 0

    def side(level):
        return jnp.where(xi == 0, level.n - 1, 0)

    def copy_x(level, colour, j):
        span = rows(j * level.width, level.width)
        k = colour * level.chunks + j
        return pltpu.make_async_remote_copy(
            src_ref=level.fx[colour].at[span], dst_ref=level.hx[colour].at[span],
            send_sem=level.sems['sx'].at[k], recv_sem=level.sems['rx'].at[k],
            device_id={'x': 1 - xi}, device_id_type=MESH)

    def copy_z(level, colour, j):
        offset = TILE + j * level.width
        src = jnp.where(zi == 0, level.planes, 1) * level.pitch + offset
        dst = jnp.where(zi == 0, 0, level.planes + 1) * level.pitch + offset
        k = colour * level.chunks + j
        return pltpu.make_async_remote_copy(
            src_ref=level.v[colour].at[rows(src, level.width)], dst_ref=level.v[colour].at[rows(dst, level.width)],
            send_sem=level.sems['sz'].at[k], recv_sem=level.sems['rz'].at[k],
            device_id={'z': 1 - zi}, device_id_type=MESH)

    def copy_y(level, colour):
        return pltpu.make_async_remote_copy(
            src_ref=level.fy[colour], dst_ref=level.hy[colour],
            send_sem=level.sems['sy'].at[colour], recv_sem=level.sems['ry'].at[colour],
            device_id={'y': 1 - yi}, device_id_type=MESH)

    def wait_y(level, colour):
        copy_y(level, colour).wait()
        ghost = jnp.where(yi == 0, level.n, -1)
        level.v[colour][pl.ds(level.pitch + TILE + ghost, level.planes, stride=level.pitch), :] = level.hy[colour][...]

    def wait_all(level, colour):
        wait_y(level, colour)

        def step(j, carry):
            copy_x(level, colour, j).wait()
            copy_z(level, colour, j).wait()
            return carry
        lax.fori_loop(0, level.chunks, step, 0)

    def fill_ghosts(level, colour):
        own, other = level.v[colour], level.v[1 - colour]
        pitch, n = level.pitch, level.n

        def fill_row(src, dst):
            if level.planes >= TILE:
                values = own[pl.ds(pitch + TILE + src, level.planes, stride=pitch), :]
                other[pl.ds(pitch + TILE + dst, level.planes, stride=pitch), :] = -values
            else:
                for k in range(level.planes):
                    base = (k + 1) * pitch + TILE
                    other[pl.ds(base + dst, 1), :] = -own[pl.ds(base + src, 1), :]

        def fill_plane(src, dst):
            other[rows(dst * pitch + TILE, level.nb), :] = -own[rows(src * pitch + TILE, level.nb), :]

        if level.dist:
            fill_row(jnp.where(yi == 0, 0, n - 1), jnp.where(yi == 0, -1, n))
            fill_plane(jnp.where(zi == 0, 1, level.planes), jnp.where(zi == 0, 0, level.planes + 1))
        else:
            fill_row(0, -1)
            fill_row(n - 1, n)
            fill_plane(1, 0)
            fill_plane(level.planes, level.planes + 1)

    def half_sweep(level, colour, mode):
        own, other, source = level.v[colour], level.v[1 - colour], level.g[colour]
        width, pitch, n, planes = level.width, level.pitch, level.n, level.planes
        stencil = mode in ('gs', 'res0', 'res1')
        sends = level.dist and mode in ('gs', 'zero', 'copy')
        waits = level.dist and mode in ('gs', 'res0')
        if stencil:
            fill_ghosts(level, colour)
        if waits:
            wait_y(level, 1 - colour)
        lane = lanes(width)
        even = even_mask(width)
        takes_below = even if colour == RED else jnp.logical_not(even)
        first_lane, last_lane = lane == 0, lane == n - 1
        if level.dist:
            q = side(level)
            halo_lane = lane == q

        def chunk(jj, carry):
            j = jnp.where(yi == 1, jj, level.chunks - 1 - jj) if level.dist else jj
            if waits:
                copy_x(level, 1 - colour, j).wait()
                copy_z(level, 1 - colour, j).wait()
            row0 = j * width + TILE
            if stencil and level.dist:
                halo = level.hx[1 - colour][rows(j * width, width), :]

            def planes_step(i, state):
                below, here, face = state
                for u in range(level.unroll):
                    k = i * level.unroll + u
                    base = (k + 1) * pitch + row0
                    if mode != 'zero':
                        old = own[rows(base, width), :]
                    if mode == 'copy':
                        new = old
                    elif mode == 'zero':
                        new = source[rows(k * level.nb + j * width, width), :] * SIXTH
                    else:
                        above = other[rows(base + pitch, width), :]
                        total = other[pl.ds(base - 1, width), :] + other[pl.ds(base + 1, width), :]
                        edge_values = -old
                        if level.dist:
                            shift = lax.rem(q - k + LANES, LANES)
                            edge_values = jnp.where(halo_lane, pltpu.roll(halo, shift, 1), edge_values)
                        left = jnp.where(first_lane, edge_values, pltpu.roll(here, 1, 1))
                        right = jnp.where(last_lane, edge_values, pltpu.roll(here, 127, 1))
                        total = total + (left + right) + (here + jnp.where(takes_below, below, above))
                        total = total + source[rows(k * level.nb + j * width, width), :]
                        new = total * SIXTH if mode == 'gs' else total - 6.0 * old
                        below, here = here, above
                    if mode in ('gs', 'zero'):
                        own[rows(base, width), :] = new
                    elif mode == 'res0':
                        refs['stage_u'][rows(k * level.nb + j * width, width), :] = new
                    elif mode == 'res1':
                        span = rows(k * level.nb + j * width, width)
                        refs['stage_u'][span, :] = refs['stage_u'][span, :] + new
                    if sends:
                        face = jnp.where(lane == k, pltpu.roll(new, lax.rem(k - q + LANES, LANES), 1), face)
                return below, here, face

            blank = jnp.zeros((width, LANES), F32)
            if stencil:
                start = (other[rows(row0, width), :], other[rows(pitch + row0, width), :], blank)
            else:
                start = (blank, blank, blank)
            _, _, face = lax.fori_loop(0, planes // level.unroll, planes_step, start)
            if sends:
                level.fx[colour][rows(j * width, width), :] = face
                copy_x(level, colour, j).start()
                copy_z(level, colour, j).start()

                @pl.when(jj == 0)
                def _():
                    y_row = jnp.where(yi == 0, n - 1, 0)
                    level.fy[colour][...] = own[pl.ds(pitch + TILE + y_row, planes, stride=pitch), :]
                    copy_y(level, colour).start()
            return carry

        lax.fori_loop(0, level.chunks, chunk, 0)

    def sweeps(level, count):
        def step(index, carry):
            half_sweep(level, RED, 'gs')
            half_sweep(level, BLACK, 'gs')
            return carry
        lax.fori_loop(0, count, step, 0)

    square_i = lax.broadcasted_iota(jnp.int32, (LANES, LANES), 0)
    square_f = lax.broadcasted_iota(jnp.int32, (LANES, LANES), 1)

    def restriction_matrix(n_coarse):
        hit = (lax.div(square_i, 2) == square_f) & (square_i < 2 * n_coarse)
        return jnp.where(hit, 0.5, 0.0).astype(F32)

    def prolongation_matrix(n_fine, n_coarse, offset, low_lane, high_lane):
        own_index = lax.div(square_f, 2) + offset
        near = jnp.where(lax.rem(square_f, 2) == 0, own_index - 1, own_index + 1)
        outside = (near < 0) | (near > n_coarse - 1)
        value = jnp.where(square_i == own_index, jnp.where(outside & (low_lane is None), 0.5, 0.75), 0.0)
        value = value + jnp.where((square_i == near) & jnp.logical_not(outside), 0.25, 0.0)
        return jnp.where(square_f < n_fine, value, 0.0).astype(F32)

    def distributed_matrix(n_coarse):
        own_index = lax.div(square_f, 2)
        near = jnp.where(lax.rem(square_f, 2) == 0, own_index - 1, own_index + 1)
        halo_near = jnp.where(xi == 0, n_coarse, -1)
        ghost_near = jnp.where(xi == 0, -1, n_coarse)
        lane_of_near = jnp.where(near == -1, 127, near)
        value = jnp.where(square_i == own_index, jnp.where(near == ghost_near, 0.5, 0.75), 0.0)
        inside = (near >= 0) & (near < n_coarse)
        value = value + jnp.where((square_i == lane_of_near) & (inside | (near == halo_near)), 0.25, 0.0)
        return value.astype(F32)

    def matmul(a, b):
        return jnp.dot(a, b, precision=HIGHEST, preferred_element_type=F32)

    stage_u, stage_f = refs['stage_u'], refs['stage_f']

    def restrict_pair(level, k, matrix):
        n_coarse = level.n // 2
        size = max(n_coarse, TILE)
        pair = []
        for z in (0, 1):
            base = (2 * k + z) * level.nb
            total = stage_u[pl.ds(base, size, stride=2), :] + stage_u[pl.ds(base + 1, size, stride=2), :]
            pair.append(matmul(total, matrix))
        even = even_mask(size)
        return jnp.where(even, pair[0], pair[1]), jnp.where(even, pair[1], pair[0])

    def restrict_local(level, coarse, index):
        matrix = refs[f'mat_q{index}'][...]

        def step(k, carry):
            red, black = restrict_pair(level, k, matrix)
            coarse.g[RED][rows(k * coarse.nb, coarse.nb), :] = red
            coarse.g[BLACK][rows(k * coarse.nb, coarse.nb), :] = black
            return carry
        lax.fori_loop(0, coarse.planes, step, 0)

    gather_own, gather_other = refs['gather_own'], refs['gather_other']
    fine_block = levels[1]
    block_n = fine_block.n // 2
    block_rows = (block_n // 4) * block_n
    slot = 2 * zi + yi

    def gather_copies():
        copies = []
        for index, flips in enumerate(((0, 1), (1, 0), (1, 1))):
            target = {'z': zi + flips[0] - 2 * zi * flips[0], 'y': yi + flips[1] - 2 * yi * flips[1]}
            here = gather_own.at[rows(slot * block_rows, block_rows)]
            copies.append(pltpu.make_async_remote_copy(
                src_ref=here, dst_ref=here, send_sem=refs['gs'].at[index], recv_sem=refs['gr'].at[index],
                device_id=target, device_id_type=MESH))
        return copies

    def partner_copy(index):
        flips = ((0, 0), (0, 1), (1, 0), (1, 1))[index]
        z = zi + flips[0] - 2 * zi * flips[0]
        y = yi + flips[1] - 2 * yi * flips[1]
        span = rows((2 * z + y) * block_rows, block_rows)
        return pltpu.make_async_remote_copy(
            src_ref=gather_own.at[span], dst_ref=gather_other.at[span],
            send_sem=refs['ps'].at[index], recv_sem=refs['pr'].at[index],
            device_id={'x': 1 - xi}, device_id_type=MESH)

    def restrict_gather(coarse):
        matrix = refs['mat_q1'][...]

        def step(m, carry):
            packed = None
            for half in (0, 1):
                for colour, part in enumerate(restrict_pair(fine_block, 2 * m + half, matrix)):
                    turn = (2 * half + colour) * block_n
                    part = part if turn == 0 else pltpu.roll(part, turn, 1)
                    packed = part if packed is None else packed + part
            gather_own[rows(slot * block_rows + m * block_n, block_n), :] = packed
            return carry
        lax.fori_loop(0, block_n // 4, step, 0)
        copies = gather_copies()
        for copy in copies:
            copy.start()
        partner_copy(0).start()
        for index, copy in enumerate(copies):
            copy.wait()
            partner_copy(index + 1).start()
        for index in range(4):
            partner_copy(index).wait()
        lane = lanes(block_n)
        low, middle = lane < block_n, lane < 2 * block_n

        for source_slot in range(4):
            zs, ys = source_slot // 2, source_slot % 2

            def unpack(m, carry):
                span = rows(source_slot * block_rows + m * block_n, block_n)
                mine, theirs = gather_own[span, :], gather_other[span, :]
                at_zero = jnp.where(xi == 0, mine, theirs)
                at_one = jnp.where(xi == 0, theirs, mine)
                for group in range(4):
                    half, colour = group // 2, group % 2
                    left = at_zero if group == 0 else pltpu.roll(at_zero, LANES - group * block_n, 1)
                    turn = (LANES - group * block_n + block_n) % LANES
                    right = at_one if turn == 0 else pltpu.roll(at_one, turn, 1)
                    value = jnp.where(low, left, jnp.where(middle, right, 0.0))
                    plane = zs * (block_n // 2) + 2 * m + half
                    coarse.g[colour][rows(plane * coarse.nb + ys * block_n, block_n), :] = value
                return carry
            lax.fori_loop(0, block_n // 4, unpack, 0)

    def set_zero(ref, size):
        def step(i, carry):
            ref[rows(i * TILE, TILE), :] = jnp.zeros((TILE, LANES), F32)
            return carry
        lax.fori_loop(0, size // TILE, step, 0)

    def expand_x(coarse, planes_ref, matrix):
        nb, pitch = coarse.nb, coarse.pitch
        lane = lanes(nb)
        even = even_mask(nb)
        keep = lane < coarse.n
        if coarse.dist:
            q = side(coarse)
            halo_lane = lane == jnp.where(xi == 0, coarse.n, 127)
            target_lane = jnp.where(xi == 0, coarse.n, 127)
            halos = [coarse.hx[colour][...] for colour in (RED, BLACK)]

        def step(k, carry):
            parts = []
            for colour in (RED, BLACK):
                value = jnp.where(keep, coarse.v[colour][rows((k + 1) * pitch + TILE, nb), :], 0.0)
                if coarse.dist:
                    rolled = pltpu.roll(halos[colour], lax.rem(target_lane - k + LANES, LANES), 1)
                    value = jnp.where(halo_lane, rolled, value)
                parts.append(value)
            red, black = parts
            planes_ref[rows((2 * k + 1) * pitch + TILE, nb), :] = matmul(jnp.where(even, red, black), matrix)
            planes_ref[rows((2 * k + 2) * pitch + TILE, nb), :] = matmul(jnp.where(even, black, red), matrix)
            return carry
        lax.fori_loop(0, coarse.planes, step, 0)

    def negate_row(ref, src, dst):
        ref[pl.ds(dst, 1), :] = -ref[pl.ds(src, 1), :]

    def pad_local(coarse, planes_ref):
        n, pitch = coarse.n, coarse.pitch
        if n >= TILE:
            for src, dst in ((0, -1), (n - 1, n)):
                values = planes_ref[pl.ds(pitch + TILE + src, n, stride=pitch), :]
                planes_ref[pl.ds(pitch + TILE + dst, n, stride=pitch), :] = -values
        else:
            for k in range(1, n + 1):
                negate_row(planes_ref, k * pitch + TILE, k * pitch + 7)
                negate_row(planes_ref, k * pitch + TILE + n - 1, k * pitch + TILE + n)
        planes_ref[rows(0, pitch), :] = -planes_ref[rows(pitch, pitch), :]
        planes_ref[rows((n + 1) * pitch, pitch), :] = -planes_ref[rows(n * pitch, pitch), :]

    def pad_distributed(coarse, planes_ref):
        n, pitch = coarse.n, coarse.pitch
        y_own = jnp.where(yi == 0, n - 1, 0)
        y_halo = jnp.where(yi == 0, n, -1)
        z_own = jnp.where(zi == 0, n, 1)
        z_halo_mine = jnp.where(zi == 0, n + 1, 0)
        z_halo_theirs = jnp.where(zi == 0, 0, n + 1)
        refs['pfy'][...] = planes_ref[pl.ds(pitch + TILE + y_own, n, stride=pitch), :]
        copy_rows = pltpu.make_async_remote_copy(
            src_ref=refs['pfy'], dst_ref=refs['phy'], send_sem=refs['qs'].at[0], recv_sem=refs['qr'].at[0],
            device_id={'y': 1 - yi}, device_id_type=MESH)
        copy_plane = pltpu.make_async_remote_copy(
            src_ref=planes_ref.at[rows(z_own * pitch + TILE, n)], dst_ref=planes_ref.at[rows(z_halo_theirs * pitch + TILE, n)],
            send_sem=refs['qs'].at[1], recv_sem=refs['qr'].at[1],
            device_id={'z': 1 - zi}, device_id_type=MESH)
        corner = z_own * pitch + TILE + jnp.where(yi == 0, n - TILE, 0)
        copy_corner = pltpu.make_async_remote_copy(
            src_ref=planes_ref.at[rows(corner, TILE)], dst_ref=refs['phc'],
            send_sem=refs['qs'].at[2], recv_sem=refs['qr'].at[2],
            device_id={'z': 1 - zi, 'y': 1 - yi}, device_id_type=MESH)
        copy_rows.start()
        copy_plane.start()
        copy_corner.start()
        ghost_src, ghost_dst = jnp.where(yi == 0, 0, n - 1), jnp.where(yi == 0, -1, n)
        values = planes_ref[pl.ds(pitch + TILE + ghost_src, n, stride=pitch), :]
        planes_ref[pl.ds(pitch + TILE + ghost_dst, n, stride=pitch), :] = -values
        copy_rows.wait()
        planes_ref[pl.ds(pitch + TILE + y_halo, n, stride=pitch), :] = refs['phy'][...]
        copy_plane.wait()
        base = z_halo_mine * pitch + TILE
        negate_row(planes_ref, base + ghost_src, base + ghost_dst)
        copy_corner.wait()
        planes_ref[pl.ds(base + y_halo, 1), :] = refs['phc'][pl.ds(jnp.where(yi == 0, 0, 7), 1), :]
        z_edge, z_ghost = jnp.where(zi == 0, 1, n), jnp.where(zi == 0, 0, n + 1)
        planes_ref[rows(z_ghost * pitch, pitch), :] = -planes_ref[rows(z_edge * pitch, pitch), :]

    def expand_zy(coarse, planes_ref, fine, z_offset, y_offset):
        half = fine.n // 2
        size = half
        pitch = coarse.pitch
        even_lane = lax.rem(lanes(size), 2) == 0

        def step(k, carry):
            middle = (k + z_offset + 1) * pitch + TILE + y_offset
            low, high = {}, {}
            for dy in (-1, 0, 1):
                here = 0.75 * planes_ref[pl.ds(middle + dy, size), :]
                low[dy] = here + 0.25 * planes_ref[pl.ds(middle - pitch + dy, size), :]
                high[dy] = here + 0.25 * planes_ref[pl.ds(middle + pitch + dy, size), :]
            for odd in (0, 1):
                dy = 2 * odd - 1
                z_even = 0.75 * low[0] + 0.25 * low[dy]
                z_odd = 0.75 * high[0] + 0.25 * high[dy]
                first = jnp.where(even_lane, z_even, z_odd)
                second = jnp.where(even_lane, z_odd, z_even)
                red, black = (first, second) if odd == 0 else (second, first)
                span = pl.ds((k + 1) * fine.pitch + TILE + odd, size, stride=2)
                fine.v[RED][span, :] = fine.v[RED][span, :] + red
                fine.v[BLACK][span, :] = fine.v[BLACK][span, :] + black
            return carry
        lax.fori_loop(0, fine.planes, step, 0)

    barrier = pltpu.get_barrier_semaphore()
    for target in ({'x': 1 - xi}, {'y': 1 - yi}, {'z': 1 - zi}, {'z': 1 - zi, 'y': 1 - yi}):
        pl.semaphore_signal(barrier, inc=1, device_id=target, device_id_type=MESH)
    pl.semaphore_wait(barrier, 4)

    top = levels[0]
    load_chunks = 4
    chunk_rows = edge * edge // load_chunks

    def load_copy(index, which):
        span = rows(index * chunk_rows, chunk_rows)
        return pltpu.make_async_copy(
            (refs['u_in'], refs['f_in'])[which].at[span], (stage_u, stage_f)[which].at[span],
            refs['load'].at[2 * index + which])

    for index in range(load_chunks):
        for which in (0, 1):
            load_copy(index, which).start()
    even_edge = even_mask(edge)
    scale = 1.0 / float((2 * edge) ** 2)

    def pack(index, carry):
        load_copy(index, 0).wait()
        load_copy(index, 1).wait()

        def step(i, inner):
            k = index * (top.planes // load_chunks) + i
            a, b = stage_u[rows(2 * k * edge, edge), :], stage_u[rows((2 * k + 1) * edge, edge), :]
            top.v[RED][rows((k + 1) * top.pitch + TILE, edge), :] = jnp.where(even_edge, a, b)
            top.v[BLACK][rows((k + 1) * top.pitch + TILE, edge), :] = jnp.where(even_edge, b, a)
            a = stage_f[rows(2 * k * edge, edge), :] * scale
            b = stage_f[rows((2 * k + 1) * edge, edge), :] * scale
            top.g[RED][rows(k * edge, edge), :] = jnp.where(even_edge, a, b)
            top.g[BLACK][rows(k * edge, edge), :] = jnp.where(even_edge, b, a)
            return inner
        return lax.fori_loop(0, top.planes // load_chunks, step, carry)
    lax.fori_loop(0, load_chunks, pack, 0)

    for index in range(len(levels) - 1):
        refs[f'mat_q{index}'][...] = restriction_matrix(levels[index].n // 2)
    refs['mat_p0'][...] = distributed_matrix(levels[1].n)
    refs['mat_p1'][...] = prolongation_matrix(levels[1].n, levels[2].n, xi * (levels[2].n // 2), None, None)
    for index in range(2, len(levels) - 1):
        fine_n = levels[index].n
        refs[f'mat_p{index}'][...] = prolongation_matrix(fine_n, fine_n // 2, 0, None, None)

    planes_dist, planes_local = refs['planes_dist'], refs['planes_local']

    def residual(level):
        half_sweep(level, RED, 'res0')
        half_sweep(level, BLACK, 'res1')

    def start_zero(level):
        set_zero(level.v[BLACK], (level.planes + 2) * level.pitch)
        half_sweep(level, RED, 'zero')
        half_sweep(level, BLACK, 'gs')
        sweeps(level, 1)

    def solve_local(index):
        level = levels[index]
        if index == len(levels) - 1:
            set_zero(level.v[BLACK], (level.planes + 2) * level.pitch)
            half_sweep(level, RED, 'zero')
            half_sweep(level, BLACK, 'gs')
            sweeps(level, COARSE_SWEEPS - 1)
            return
        start_zero(level)
        residual(level)
        restrict_local(level, levels[index + 1], index)
        solve_local(index + 1)
        expand_x(levels[index + 1], planes_local, refs[f'mat_p{index}'][...])
        pad_local(levels[index + 1], planes_local)
        expand_zy(levels[index + 1], planes_local, level, 0, 0)
        sweeps(level, 2)

    half_sweep(top, BLACK, 'copy')

    def cycle(index, carry):
        middle = levels[1]
        sweeps(top, 2)
        residual(top)
        restrict_local(top, middle, 0)
        start_zero(middle)
        residual(middle)
        restrict_gather(levels[2])
        solve_local(2)
        expand_x(levels[2], planes_local, refs['mat_p1'][...])
        pad_local(levels[2], planes_local)
        expand_zy(levels[2], planes_local, middle, zi * (levels[2].n // 2), yi * (levels[2].n // 2))
        half_sweep(middle, BLACK, 'copy')
        sweeps(middle, 2)
        wait_all(middle, BLACK)
        expand_x(middle, planes_dist, refs['mat_p0'][...])
        pad_distributed(middle, planes_dist)
        expand_zy(middle, planes_dist, top, 0, 0)
        half_sweep(top, BLACK, 'copy')
        sweeps(top, 2)
        return carry
    lax.fori_loop(0, CYCLES, cycle, 0)
    wait_all(top, BLACK)

    def store_copy(k, colour):
        return pltpu.make_async_copy(
            top.v[colour].at[rows((k + 1) * top.pitch + TILE, edge)],
            (refs['red_out'], refs['black_out'])[colour].at[rows(k * edge, edge)], refs['store'].at[2 * k + colour])

    def store_start(k, carry):
        store_copy(k, RED).start()
        store_copy(k, BLACK).start()
        return carry

    def store_wait(k, carry):
        store_copy(k, RED).wait()
        store_copy(k, BLACK).wait()
        return carry
    lax.fori_loop(0, top.planes, store_start, 0)
    lax.fori_loop(0, top.planes, store_wait, 0)


def solve_packed(initial, source, edge):
    levels = make_levels(edge)
    names = ['u_in', 'f_in', 'red_out', 'black_out']
    scratch = []

    def add(name, shape):
        names.append(name)
        scratch.append(shape)

    for index, level in enumerate(levels):
        for key, shape in level.scratch().items():
            add(f'L{index}_{key}', shape)
    add('stage_u', pltpu.VMEM((edge * edge, LANES), F32))
    add('stage_f', pltpu.VMEM((edge * edge, LANES), F32))
    for index in range(len(levels) - 1):
        add(f'mat_p{index}', pltpu.VMEM((LANES, LANES), F32))
        add(f'mat_q{index}', pltpu.VMEM((LANES, LANES), F32))
    middle, replicated = levels[1], levels[2]
    add('planes_dist', pltpu.VMEM(((middle.n + 2) * middle.pitch, LANES), F32))
    add('planes_local', pltpu.VMEM(((replicated.n + 2) * replicated.pitch, LANES), F32))
    add('pfy', pltpu.VMEM((middle.n, LANES), F32))
    add('phy', pltpu.VMEM((middle.n, LANES), F32))
    add('phc', pltpu.VMEM((TILE, LANES), F32))
    add('qs', pltpu.SemaphoreType.DMA((3,)))
    add('qr', pltpu.SemaphoreType.DMA((3,)))
    block_n = middle.n // 2
    add('gather_own', pltpu.VMEM((4 * (block_n // 4) * block_n, LANES), F32))
    add('gather_other', pltpu.VMEM((4 * (block_n // 4) * block_n, LANES), F32))
    add('gs', pltpu.SemaphoreType.DMA((3,)))
    add('gr', pltpu.SemaphoreType.DMA((3,)))
    add('ps', pltpu.SemaphoreType.DMA((4,)))
    add('pr', pltpu.SemaphoreType.DMA((4,)))
    add('load', pltpu.SemaphoreType.DMA((TILE,)))
    add('store', pltpu.SemaphoreType.DMA((edge,)))
    half = jax.ShapeDtypeStruct((edge * edge // 2, LANES), F32)
    return pl.pallas_call(
        functools.partial(kernel_body, names, edge),
        out_shape=(half, half),
        in_specs=[pl.BlockSpec(memory_space=pl.ANY)] * 2,
        out_specs=(pl.BlockSpec(memory_space=pl.ANY),) * 2,
        scratch_shapes=scratch,
        compiler_params=pltpu.CompilerParams(collective_id=0, has_side_effects=True, vmem_limit_bytes=66000000),
        name='multigrid',
    )(initial, source)


def unpack_body(red_ref, black_ref, out_ref):
    planes = red_ref.shape[0]
    even = lax.rem(lax.broadcasted_iota(jnp.int32, (LANES, LANES), 0) + lax.broadcasted_iota(jnp.int32, (LANES, LANES), 1), 2) == 0
    for k in range(planes):
        red, black = red_ref[k], black_ref[k]
        out_ref[2 * k] = jnp.where(even, red, black)
        out_ref[2 * k + 1] = jnp.where(even, black, red)


def unpack(red, black, edge):
    step = TILE
    spec = pl.BlockSpec((step, edge, LANES), lambda i: (i, 0, 0))
    return pl.pallas_call(
        unpack_body,
        grid=(edge // 2 // step,),
        out_shape=jax.ShapeDtypeStruct((edge, edge, LANES), F32),
        in_specs=[spec, spec],
        out_specs=pl.BlockSpec((2 * step, edge, LANES), lambda i: (i, 0, 0)),
        name='unpack',
    )(red.reshape(edge // 2, edge, LANES), black.reshape(edge // 2, edge, LANES))


def solution(mesh):
    grid_spec = P(('batch', 'z'), 'y', 'x')

    def local_solve(source, initial_guess):
        edge = source.shape[0]
        red, black = solve_packed(
            initial_guess.reshape(edge * edge, edge), source.reshape(edge * edge, edge), edge)
        return unpack(red, black, edge)

    return jax.shard_map(local_solve, mesh=mesh, in_specs=(grid_spec, grid_spec), out_specs=grid_spec, check_vma=False)
```

```python
import functools

import jax
import jax.numpy as jnp
from jax import lax
from jax.experimental import pallas as pl
from jax.experimental.pallas import tpu as pltpu
from jax.sharding import PartitionSpec as P

CYCLES = 2
COARSE_SWEEPS = 24
LANES = 128
WIDTH = 32
GROUP = 4
TILE = 8
MESH = pl.DeviceIdType.MESH
F32 = jnp.float32
SIXTH = 1.0 / 6.0
RED, BLACK = 0, 1
HIGHEST = lax.Precision.HIGHEST


def mult8(value):
    return value if isinstance(value, int) else pl.multiple_of(value, TILE)


def rows(start, size):
    return pl.ds(mult8(start), size)


class Level:
    def __init__(self, n, dist, width, unroll):
        self.n = n
        self.planes = n // 2
        self.nb = max(n, TILE)
        self.pitch = self.nb + 16
        self.dist = dist
        self.width = min(width, self.nb)
        self.chunks = self.nb // self.width
        self.unroll = min(unroll, self.planes)

    def scratch(self):
        cells = pltpu.VMEM(((self.planes + 2) * self.pitch, LANES), F32)
        packed = pltpu.VMEM((self.planes * self.nb, LANES), F32)
        shapes = dict(v0=cells, v1=cells, g0=packed, g1=packed)
        if self.dist:
            face_x = pltpu.VMEM((self.nb, LANES), F32)
            face_y = pltpu.VMEM((self.planes, LANES), F32)
            for colour in (RED, BLACK):
                shapes[f'fx{colour}'] = face_x
                shapes[f'hx{colour}'] = face_x
                shapes[f'fy{colour}'] = face_y
                shapes[f'hy{colour}'] = face_y
            for axis in ('x', 'z'):
                shapes[f's{axis}'] = pltpu.SemaphoreType.DMA((2 * self.chunks,))
                shapes[f'r{axis}'] = pltpu.SemaphoreType.DMA((2 * self.chunks,))
            shapes['sy'] = pltpu.SemaphoreType.DMA((2,))
            shapes['ry'] = pltpu.SemaphoreType.DMA((2,))
        return shapes

    def bind(self, refs):
        self.v = (refs['v0'], refs['v1'])
        self.g = (refs['g0'], refs['g1'])
        if self.dist:
            self.fx = (refs['fx0'], refs['fx1'])
            self.hx = (refs['hx0'], refs['hx1'])
            self.fy = (refs['fy0'], refs['fy1'])
            self.hy = (refs['hy0'], refs['hy1'])
            self.sems = {key: refs[key] for key in ('sx', 'rx', 'sz', 'rz', 'sy', 'ry')}


def make_levels(edge):
    levels = [Level(edge, True, WIDTH, 16), Level(edge // 2, True, WIDTH, 8)]
    n = edge // 2
    while n >= 4:
        levels.append(Level(n, False, 2 * WIDTH, 8))
        n = n // 2
    return levels


def kernel_body(names, edge, *args):
    refs = dict(zip(names, args))
    xi, yi, zi = lax.axis_index('x'), lax.axis_index('y'), lax.axis_index('z')
    levels = make_levels(edge)
    for index, level in enumerate(levels):
        prefix = f'L{index}_'
        level.bind({key[len(prefix):]: ref for key, ref in refs.items() if key.startswith(prefix)})

    def lanes(size):
        return lax.broadcasted_iota(jnp.int32, (size, LANES), 1)

    def even_mask(size):
        return lax.rem(lanes(size) + lax.broadcasted_iota(jnp.int32, (size, LANES), 0), 2) == 0

    def side(level):
        return jnp.where(xi == 0, level.n - 1, 0)

    def turn(value, shift):
        return pltpu.roll(value, lax.rem(shift + 2 * LANES, LANES), 1)

    def skew(level, k):
        return k + level.planes * zi if level.dist else k

    def copy_x(level, colour, j):
        span = rows(j * level.width, level.width)
        k = colour * level.chunks + j
        return pltpu.make_async_remote_copy(
            src_ref=level.fx[colour].at[span], dst_ref=level.hx[colour].at[span],
            send_sem=level.sems['sx'].at[k], recv_sem=level.sems['rx'].at[k],
            device_id={'x': 1 - xi}, device_id_type=MESH)

    def copy_z(level, colour, j):
        offset = TILE + j * level.width
        src = jnp.where(zi == 0, level.planes, 1) * level.pitch + offset
        dst = jnp.where(zi == 0, 0, level.planes + 1) * level.pitch + offset
        k = colour * level.chunks + j
        return pltpu.make_async_remote_copy(
            src_ref=level.v[colour].at[rows(src, level.width)], dst_ref=level.v[colour].at[rows(dst, level.width)],
            send_sem=level.sems['sz'].at[k], recv_sem=level.sems['rz'].at[k],
            device_id={'z': 1 - zi}, device_id_type=MESH)

    def copy_y(level, colour):
        return pltpu.make_async_remote_copy(
            src_ref=level.fy[colour], dst_ref=level.hy[colour],
            send_sem=level.sems['sy'].at[colour], recv_sem=level.sems['ry'].at[colour],
            device_id={'y': 1 - yi}, device_id_type=MESH)

    def wait_y(level, colour):
        copy_y(level, colour).wait()
        ghost = jnp.where(yi == 0, level.n, -1)
        level.v[colour][pl.ds(level.pitch + TILE + ghost, level.planes, stride=level.pitch), :] = level.hy[colour][...]

    def wait_all(level, colour):
        wait_y(level, colour)

        def step(j, carry):
            copy_x(level, colour, j).wait()
            copy_z(level, colour, j).wait()
            return carry
        lax.fori_loop(0, level.chunks, step, 0)

    stage_u, stage_f = refs['stage_u'], refs['stage_f']

    def fill_ghosts(level, colour):
        own, other = level.v[colour], level.v[1 - colour]
        pitch, n = level.pitch, level.n

        def fill_row(src, dst):
            if level.planes >= TILE:
                values = own[pl.ds(pitch + TILE + src, level.planes, stride=pitch), :]
                other[pl.ds(pitch + TILE + dst, level.planes, stride=pitch), :] = -values
            else:
                for k in range(level.planes):
                    base = (k + 1) * pitch + TILE
                    other[pl.ds(base + dst, 1), :] = -own[pl.ds(base + src, 1), :]

        if level.dist:
            fill_row(jnp.where(yi == 0, 0, n - 1), jnp.where(yi == 0, -1, n))
        else:
            fill_row(0, -1)
            fill_row(n - 1, n)

    def half_sweep(level, colour, mode):
        own, other, source = level.v[colour], level.v[1 - colour], level.g[colour]
        width, pitch, n, planes = level.width, level.pitch, level.n, level.planes
        stencil = mode in ('gs', 'res0', 'res1')
        sends = level.dist and mode in ('gs', 'zero', 'copy')
        waits = level.dist and mode in ('gs', 'res0')
        if stencil:
            fill_ghosts(level, colour)
        if waits:
            wait_y(level, 1 - colour)
        lane = lanes(width)
        even = even_mask(width)
        odd = jnp.logical_not(even)
        takes_below = (even, odd) if colour == RED else (odd, even)
        q = side(level)

        def chunk(jj, carry):
            j = jnp.where(yi == 1, jj, level.chunks - 1 - jj) if level.dist else jj
            if waits:
                copy_x(level, 1 - colour, j).wait()
                copy_z(level, 1 - colour, j).wait()
            row0 = j * width + TILE
            blank = jnp.zeros((width, LANES), F32)
            unroll = level.unroll
            steps = planes // unroll
            pair_sum = refs['pair_sum']
            if stencil and level.dist:
                halo = level.hx[1 - colour][rows(j * width, width), :]

            def load(ref, start):
                return ref[rows(start, width), :]

            def turned(start):
                here = load(other, start)
                return pltpu.roll(here, 1, 1), pltpu.roll(here, LANES - 1, 1)

            def ghost(start, rotated, outside):
                minus = -load(own, start)
                return minus if rotated is None else jnp.where(outside, minus, rotated)

            def at(place):
                return lane == lax.rem(place, LANES)

            def along_x(start, place, left, right):
                ends = -load(own, start)
                if level.dist:
                    ends = lax.select(at(place + q), halo, ends)
                return lax.select(at(place), ends, left) + lax.select(at(place + (n - 1)), ends, right)

            def across(i, state):
                older, newer, sums = state
                start = (i * unroll + 1) * pitch + row0
                place = skew(level, i * unroll)
                final = i == steps - 1
                for u in range(unroll):
                    left, right = turned(start + (u + 1) * pitch)
                    following = start + (u + 1) * pitch
                    if u == unroll - 1:
                        outside = final & (zi == 1) if level.dist else final
                        right = ghost(start + u * pitch, right, outside)
                        following = start + jnp.where(final, u, u + 1) * pitch
                    sums = sums + lax.select(takes_below[u % 2], older, right)
                    pair_sum[rows(i * (unroll * width) + u * width, width), :] = sums
                    older, newer, sums = newer, left, along_x(following, place + (u + 1), left, right)
                return older, newer, sums

            def update(i, face):
                start = (i * unroll + 1) * pitch + row0
                place = skew(level, i * unroll) + q
                packed = i * (unroll * level.nb) + j * width
                for u in range(unroll):
                    base = start + u * pitch
                    span = rows(packed + u * level.nb, width)
                    if mode == 'copy':
                        new = load(own, base)
                    elif mode == 'zero':
                        new = source[span, :] * SIXTH
                    else:
                        total = other[pl.ds(base - 1, width), :] + other[pl.ds(base + 1, width), :]
                        total = total + load(pair_sum, i * (unroll * width) + u * width)
                        total = total + load(other, base) + source[span, :]
                        new = total * SIXTH if mode == 'gs' else total - 6.0 * load(own, base)
                    if mode in ('gs', 'zero'):
                        own[rows(base, width), :] = new
                    elif mode == 'res0':
                        stage_u[span, :] = new
                    elif mode == 'res1':
                        stage_u[span, :] = stage_u[span, :] + new
                    if sends:
                        face = lax.select(at(place + u), new, face)
                return face

            if stencil:
                first = pitch + row0
                below = ghost(first, turned(row0)[0] if level.dist else None, zi == 0)
                left, right = turned(first)
                state = across(0, (below, left, along_x(first, skew(level, 0), left, right)))

                def planes_step(i, carried):
                    state, face = carried
                    state = across(i + 1, state)
                    return state, update(i, face)
                _, face = lax.fori_loop(0, steps - 1, planes_step, (state, blank))
                face = update(steps - 1, face)
            else:
                face = lax.fori_loop(0, steps, update, blank)
            if sends:
                level.fx[colour][rows(j * width, width), :] = turn(face, (2 * xi - 1) * (n - 1))
                copy_x(level, colour, j).start()
                copy_z(level, colour, j).start()

                @pl.when(jj == 0)
                def _():
                    y_row = jnp.where(yi == 0, n - 1, 0)
                    level.fy[colour][...] = own[pl.ds(pitch + TILE + y_row, planes, stride=pitch), :]
                    copy_y(level, colour).start()
            return carry

        lax.fori_loop(0, level.chunks, chunk, 0)

    def sweeps(level, count):
        def step(index, carry):
            half_sweep(level, RED, 'gs')
            half_sweep(level, BLACK, 'gs')
            return carry
        lax.fori_loop(0, count, step, 0)

    square_i = lax.broadcasted_iota(jnp.int32, (LANES, LANES), 0)
    square_f = lax.broadcasted_iota(jnp.int32, (LANES, LANES), 1)

    def restriction_matrix(n_coarse):
        hit = (lax.div(square_i, 2) == square_f) & (square_i < 2 * n_coarse)
        return jnp.where(hit, 0.5, 0.0).astype(F32)

    def prolongation_matrix(n_fine, n_coarse, offset, low_lane, high_lane):
        own_index = lax.div(square_f, 2) + offset
        near = jnp.where(lax.rem(square_f, 2) == 0, own_index - 1, own_index + 1)
        outside = (near < 0) | (near > n_coarse - 1)
        value = jnp.where(square_i == own_index, jnp.where(outside & (low_lane is None), 0.5, 0.75), 0.0)
        value = value + jnp.where((square_i == near) & jnp.logical_not(outside), 0.25, 0.0)
        return jnp.where(square_f < n_fine, value, 0.0).astype(F32)

    def distributed_matrix(n_coarse):
        own_index = lax.div(square_f, 2)
        near = jnp.where(lax.rem(square_f, 2) == 0, own_index - 1, own_index + 1)
        halo_near = jnp.where(xi == 0, n_coarse, -1)
        ghost_near = jnp.where(xi == 0, -1, n_coarse)
        lane_of_near = jnp.where(near == -1, 127, near)
        value = jnp.where(square_i == own_index, jnp.where(near == ghost_near, 0.5, 0.75), 0.0)
        inside = (near >= 0) & (near < n_coarse)
        value = value + jnp.where((square_i == lane_of_near) & (inside | (near == halo_near)), 0.25, 0.0)
        return value.astype(F32)

    def matmul(a, b):
        return jnp.dot(a, b, precision=HIGHEST, preferred_element_type=F32)

    def restrict_pair(level, k, matrix):
        n_coarse = level.n // 2
        size = max(n_coarse, TILE)
        pair = []
        for z in (0, 1):
            base = (2 * k + z) * level.nb
            total = stage_u[pl.ds(base, size, stride=2), :] + stage_u[pl.ds(base + 1, size, stride=2), :]
            pair.append(matmul(turn(total, -skew(level, 2 * k + z)), matrix))
        even = even_mask(size)
        return jnp.where(even, pair[0], pair[1]), jnp.where(even, pair[1], pair[0])

    def grouped(count, size, body):
        size = min(size, count)

        def step(i, carry):
            body([i * size + u for u in range(size)])
            return carry
        lax.fori_loop(0, count // size, step, 0)

    def restrict_local(level, coarse, index):
        matrix = refs[f'mat_q{index}'][...]

        def step(indices):
            pairs = [restrict_pair(level, k, matrix) for k in indices]
            pairs = [[turn(part, skew(coarse, k)) for part in pair] for k, pair in zip(indices, pairs)]
            for k, pair in zip(indices, pairs):
                for colour in (RED, BLACK):
                    coarse.g[colour][rows(k * coarse.nb, coarse.nb), :] = pair[colour]
        grouped(coarse.planes, GROUP, step)

    gather_own, gather_other = refs['gather_own'], refs['gather_other']
    fine_block = levels[1]
    block_n = fine_block.n // 2
    block_rows = (block_n // 4) * block_n
    slot = 2 * zi + yi

    def gather_copies():
        copies = []
        for index, flips in enumerate(((0, 1), (1, 0), (1, 1))):
            target = {'z': zi + flips[0] - 2 * zi * flips[0], 'y': yi + flips[1] - 2 * yi * flips[1]}
            here = gather_own.at[rows(slot * block_rows, block_rows)]
            copies.append(pltpu.make_async_remote_copy(
                src_ref=here, dst_ref=here, send_sem=refs['gs'].at[index], recv_sem=refs['gr'].at[index],
                device_id=target, device_id_type=MESH))
        return copies

    def partner_copy(index):
        flips = ((0, 0), (0, 1), (1, 0), (1, 1))[index]
        z = zi + flips[0] - 2 * zi * flips[0]
        y = yi + flips[1] - 2 * yi * flips[1]
        span = rows((2 * z + y) * block_rows, block_rows)
        return pltpu.make_async_remote_copy(
            src_ref=gather_own.at[span], dst_ref=gather_other.at[span],
            send_sem=refs['ps'].at[index], recv_sem=refs['pr'].at[index],
            device_id={'x': 1 - xi}, device_id_type=MESH)

    def restrict_gather(coarse):
        matrix = refs['mat_q1'][...]

        def step(indices):
            for m in indices:
                packed = None
                for half in (0, 1):
                    for colour, part in enumerate(restrict_pair(fine_block, 2 * m + half, matrix)):
                        part = turn(part, (2 * half + colour) * block_n)
                        packed = part if packed is None else packed + part
                gather_own[rows(slot * block_rows + m * block_n, block_n), :] = packed
        grouped(block_n // 4, GROUP, step)
        copies = gather_copies()
        for copy in copies:
            copy.start()
        partner_copy(0).start()
        for index, copy in enumerate(copies):
            copy.wait()
            partner_copy(index + 1).start()
        for index in range(4):
            partner_copy(index).wait()
        lane = lanes(block_n)

        for source_slot in range(4):
            zs, ys = source_slot // 2, source_slot % 2

            def unpack(indices):
                results = []
                for m in indices:
                    span = rows(source_slot * block_rows + m * block_n, block_n)
                    mine, theirs = gather_own[span, :], gather_other[span, :]
                    at_zero = jnp.where(xi == 0, mine, theirs)
                    at_one = jnp.where(xi == 0, theirs, mine)
                    for group in range(4):
                        half, colour = group // 2, group % 2
                        plane = zs * (block_n // 2) + 2 * m + half
                        left = turn(at_zero, plane - group * block_n)
                        right = turn(at_one, plane + block_n - group * block_n)
                        place = lax.rem(lane + LANES - plane, LANES)
                        value = jnp.where(place < block_n, left, jnp.where(place < 2 * block_n, right, 0.0))
                        results.append((colour, plane, value))
                for colour, plane, value in results:
                    coarse.g[colour][rows(plane * coarse.nb + ys * block_n, block_n), :] = value
            grouped(block_n // 4, GROUP, unpack)

    def set_zero(ref, size):
        def step(i, carry):
            ref[rows(i * TILE, TILE), :] = jnp.zeros((TILE, LANES), F32)
            return carry
        lax.fori_loop(0, size // TILE, step, 0)

    def expand_x(coarse, planes_ref, matrix):
        nb, pitch = coarse.nb, coarse.pitch
        lane = lanes(nb)
        even = even_mask(nb)
        keep = lane < coarse.n
        if coarse.dist:
            q = side(coarse)
            halo_lane = lane == jnp.where(xi == 0, coarse.n, 127)
            target_lane = jnp.where(xi == 0, coarse.n, 127)
            halos = [coarse.hx[colour][...] for colour in (RED, BLACK)]

        def step(indices):
            results = []
            for k in indices:
                parts = []
                for colour in (RED, BLACK):
                    value = turn(coarse.v[colour][rows((k + 1) * pitch + TILE, nb), :], -skew(coarse, k))
                    value = jnp.where(keep, value, 0.0)
                    if coarse.dist:
                        halo = turn(halos[colour], target_lane - q - skew(coarse, k))
                        value = jnp.where(halo_lane, halo, value)
                    parts.append(value)
                red, black = parts
                results.append(matmul(jnp.where(even, red, black), matrix))
                results.append(matmul(jnp.where(even, black, red), matrix))
            for offset, value in enumerate(results):
                planes_ref[rows((2 * indices[0] + 1 + offset) * pitch + TILE, nb), :] = value
        grouped(coarse.planes, GROUP, step)

    def negate_row(ref, src, dst):
        ref[pl.ds(dst, 1), :] = -ref[pl.ds(src, 1), :]

    def pad_local(coarse, planes_ref):
        n, pitch = coarse.n, coarse.pitch
        if n >= TILE:
            for src, dst in ((0, -1), (n - 1, n)):
                values = planes_ref[pl.ds(pitch + TILE + src, n, stride=pitch), :]
                planes_ref[pl.ds(pitch + TILE + dst, n, stride=pitch), :] = -values
        else:
            for k in range(1, n + 1):
                negate_row(planes_ref, k * pitch + TILE, k * pitch + 7)
                negate_row(planes_ref, k * pitch + TILE + n - 1, k * pitch + TILE + n)
        planes_ref[rows(0, pitch), :] = -planes_ref[rows(pitch, pitch), :]
        planes_ref[rows((n + 1) * pitch, pitch), :] = -planes_ref[rows(n * pitch, pitch), :]

    def pad_distributed(coarse, planes_ref):
        n, pitch = coarse.n, coarse.pitch
        y_own = jnp.where(yi == 0, n - 1, 0)
        y_halo = jnp.where(yi == 0, n, -1)
        z_own = jnp.where(zi == 0, n, 1)
        z_halo_mine = jnp.where(zi == 0, n + 1, 0)
        z_halo_theirs = jnp.where(zi == 0, 0, n + 1)
        refs['pfy'][...] = planes_ref[pl.ds(pitch + TILE + y_own, n, stride=pitch), :]
        copy_rows = pltpu.make_async_remote_copy(
            src_ref=refs['pfy'], dst_ref=refs['phy'], send_sem=refs['qs'].at[0], recv_sem=refs['qr'].at[0],
            device_id={'y': 1 - yi}, device_id_type=MESH)
        copy_plane = pltpu.make_async_remote_copy(
            src_ref=planes_ref.at[rows(z_own * pitch + TILE, n)], dst_ref=planes_ref.at[rows(z_halo_theirs * pitch + TILE, n)],
            send_sem=refs['qs'].at[1], recv_sem=refs['qr'].at[1],
            device_id={'z': 1 - zi}, device_id_type=MESH)
        corner = z_own * pitch + TILE + jnp.where(yi == 0, n - TILE, 0)
        copy_corner = pltpu.make_async_remote_copy(
            src_ref=planes_ref.at[rows(corner, TILE)], dst_ref=refs['phc'],
            send_sem=refs['qs'].at[2], recv_sem=refs['qr'].at[2],
            device_id={'z': 1 - zi, 'y': 1 - yi}, device_id_type=MESH)
        copy_rows.start()
        copy_plane.start()
        copy_corner.start()
        ghost_src, ghost_dst = jnp.where(yi == 0, 0, n - 1), jnp.where(yi == 0, -1, n)
        values = planes_ref[pl.ds(pitch + TILE + ghost_src, n, stride=pitch), :]
        planes_ref[pl.ds(pitch + TILE + ghost_dst, n, stride=pitch), :] = -values
        copy_rows.wait()
        planes_ref[pl.ds(pitch + TILE + y_halo, n, stride=pitch), :] = refs['phy'][...]
        copy_plane.wait()
        base = z_halo_mine * pitch + TILE
        negate_row(planes_ref, base + ghost_src, base + ghost_dst)
        copy_corner.wait()
        planes_ref[pl.ds(base + y_halo, 1), :] = refs['phc'][pl.ds(jnp.where(yi == 0, 0, 7), 1), :]
        z_edge, z_ghost = jnp.where(zi == 0, 1, n), jnp.where(zi == 0, 0, n + 1)
        planes_ref[rows(z_ghost * pitch, pitch), :] = -planes_ref[rows(z_edge * pitch, pitch), :]

    def expand_zy(coarse, planes_ref, fine, z_offset, y_offset):
        half = fine.n // 2
        size = half
        pitch = coarse.pitch
        even_lane = lax.rem(lanes(size), 2) == 0

        def step(indices):
            results = []
            for k in indices:
                middle = (k + z_offset + 1) * pitch + TILE + y_offset
                low, high = {}, {}
                for dy in (-1, 0, 1):
                    here = 0.75 * planes_ref[pl.ds(middle + dy, size), :]
                    low[dy] = here + 0.25 * planes_ref[pl.ds(middle - pitch + dy, size), :]
                    high[dy] = here + 0.25 * planes_ref[pl.ds(middle + pitch + dy, size), :]
                for odd in (0, 1):
                    dy = 2 * odd - 1
                    z_even = 0.75 * low[0] + 0.25 * low[dy]
                    z_odd = 0.75 * high[0] + 0.25 * high[dy]
                    first = turn(jnp.where(even_lane, z_even, z_odd), skew(fine, k))
                    second = turn(jnp.where(even_lane, z_odd, z_even), skew(fine, k))
                    span = pl.ds((k + 1) * fine.pitch + TILE + odd, size, stride=2)
                    for colour, change in ((odd, first), (1 - odd, second)):
                        results.append((colour, span, fine.v[colour][span, :] + change))
            for colour, span, value in results:
                fine.v[colour][span, :] = value
        grouped(fine.planes, 2, step)

    barrier = pltpu.get_barrier_semaphore()
    for target in ({'x': 1 - xi}, {'y': 1 - yi}, {'z': 1 - zi}, {'z': 1 - zi, 'y': 1 - yi}):
        pl.semaphore_signal(barrier, inc=1, device_id=target, device_id_type=MESH)
    pl.semaphore_wait(barrier, 4)

    top = levels[0]
    load_chunks = 4
    chunk_rows = edge * edge // load_chunks

    def load_copy(index, which):
        span = rows(index * chunk_rows, chunk_rows)
        return pltpu.make_async_copy(
            (refs['u_in'], refs['f_in'])[which].at[span], (stage_u, stage_f)[which].at[span],
            refs['load'].at[2 * index + which])

    for index in range(load_chunks):
        for which in (0, 1):
            load_copy(index, which).start()
    even_edge = even_mask(edge)
    scale = 1.0 / float((2 * edge) ** 2)

    def pack(index, carry):
        load_copy(index, 0).wait()
        load_copy(index, 1).wait()

        def step(i, inner):
            k = index * (top.planes // load_chunks) + i
            a, b = stage_u[rows(2 * k * edge, edge), :], stage_u[rows((2 * k + 1) * edge, edge), :]
            top.v[RED][rows((k + 1) * top.pitch + TILE, edge), :] = turn(jnp.where(even_edge, a, b), skew(top, k))
            top.v[BLACK][rows((k + 1) * top.pitch + TILE, edge), :] = turn(jnp.where(even_edge, b, a), skew(top, k))
            a = stage_f[rows(2 * k * edge, edge), :] * scale
            b = stage_f[rows((2 * k + 1) * edge, edge), :] * scale
            top.g[RED][rows(k * edge, edge), :] = turn(jnp.where(even_edge, a, b), skew(top, k))
            top.g[BLACK][rows(k * edge, edge), :] = turn(jnp.where(even_edge, b, a), skew(top, k))
            return inner
        return lax.fori_loop(0, top.planes // load_chunks, step, carry)
    lax.fori_loop(0, load_chunks, pack, 0)

    for index in range(len(levels) - 1):
        refs[f'mat_q{index}'][...] = restriction_matrix(levels[index].n // 2)
    refs['mat_p0'][...] = distributed_matrix(levels[1].n)
    refs['mat_p1'][...] = prolongation_matrix(levels[1].n, levels[2].n, xi * (levels[2].n // 2), None, None)
    for index in range(2, len(levels) - 1):
        fine_n = levels[index].n
        refs[f'mat_p{index}'][...] = prolongation_matrix(fine_n, fine_n // 2, 0, None, None)

    planes_dist, planes_local = refs['planes_dist'], refs['planes_local']

    def residual(level):
        half_sweep(level, RED, 'res0')
        half_sweep(level, BLACK, 'res1')

    def solve(level, sweep_count, phases, descend):
        def phase(p, carry):
            def sweep(index, inner):
                fresh = (p == 0) & (index == 0)

                @pl.when(fresh)
                def _():
                    set_zero(level.v[BLACK], (level.planes + 2) * level.pitch)
                    half_sweep(level, RED, 'zero')

                @pl.when(jnp.logical_not(fresh))
                def _():
                    half_sweep(level, RED, 'gs')
                half_sweep(level, BLACK, 'gs')
                return inner
            lax.fori_loop(0, sweep_count, sweep, 0)
            if phases == 2:
                @pl.when(p == 0)
                def _():
                    residual(level)
                    descend()
            return carry
        lax.fori_loop(0, phases, phase, 0)

    def solve_local(index):
        level = levels[index]
        if index == len(levels) - 1:
            solve(level, COARSE_SWEEPS, 1, None)
            return

        def descend():
            restrict_local(level, levels[index + 1], index)
            solve_local(index + 1)
            expand_x(levels[index + 1], planes_local, refs[f'mat_p{index}'][...])
            pad_local(levels[index + 1], planes_local)
            expand_zy(levels[index + 1], planes_local, level, 0, 0)
        solve(level, 2, 2, descend)

    middle, replicated = levels[1], levels[2]

    def descend_middle():
        restrict_gather(replicated)
        solve_local(2)
        expand_x(replicated, planes_local, refs['mat_p1'][...])
        pad_local(replicated, planes_local)
        expand_zy(replicated, planes_local, middle, zi * (replicated.n // 2), yi * (replicated.n // 2))
        half_sweep(middle, BLACK, 'copy')

    half_sweep(top, BLACK, 'copy')

    def sweep_pair(index, carry):
        sweeps(top, 2)

        @pl.when(lax.rem(index, 2) == 0)
        def _():
            residual(top)
            restrict_local(top, middle, 0)
            solve(middle, 2, 2, descend_middle)
            wait_all(middle, BLACK)
            expand_x(middle, planes_dist, refs['mat_p0'][...])
            pad_distributed(middle, planes_dist)
            expand_zy(middle, planes_dist, top, 0, 0)
            half_sweep(top, BLACK, 'copy')
        return carry
    lax.fori_loop(0, 2 * CYCLES, sweep_pair, 0)
    wait_all(top, BLACK)

    def store_copy(k, colour):
        return pltpu.make_async_copy(
            top.v[colour].at[rows((k + 1) * top.pitch + TILE, edge)],
            (refs['red_out'], refs['black_out'])[colour].at[rows(k * edge, edge)], refs['store'].at[2 * k + colour])

    def store_start(k, carry):
        store_copy(k, RED).start()
        store_copy(k, BLACK).start()
        return carry

    def store_wait(k, carry):
        store_copy(k, RED).wait()
        store_copy(k, BLACK).wait()
        return carry
    lax.fori_loop(0, top.planes, store_start, 0)
    lax.fori_loop(0, top.planes, store_wait, 0)


def solve_packed(initial, source, edge):
    levels = make_levels(edge)
    names = ['u_in', 'f_in', 'red_out', 'black_out']
    scratch = []

    def add(name, shape):
        names.append(name)
        scratch.append(shape)

    for index, level in enumerate(levels):
        for key, shape in level.scratch().items():
            add(f'L{index}_{key}', shape)
    add('stage_u', pltpu.VMEM((edge * edge, LANES), F32))
    add('stage_f', pltpu.VMEM((edge * edge, LANES), F32))
    add('pair_sum', pltpu.VMEM((edge * WIDTH, LANES), F32))
    for index in range(len(levels) - 1):
        add(f'mat_p{index}', pltpu.VMEM((LANES, LANES), F32))
        add(f'mat_q{index}', pltpu.VMEM((LANES, LANES), F32))
    middle, replicated = levels[1], levels[2]
    add('planes_dist', pltpu.VMEM(((middle.n + 2) * middle.pitch, LANES), F32))
    add('planes_local', pltpu.VMEM(((replicated.n + 2) * replicated.pitch, LANES), F32))
    add('pfy', pltpu.VMEM((middle.n, LANES), F32))
    add('phy', pltpu.VMEM((middle.n, LANES), F32))
    add('phc', pltpu.VMEM((TILE, LANES), F32))
    add('qs', pltpu.SemaphoreType.DMA((3,)))
    add('qr', pltpu.SemaphoreType.DMA((3,)))
    block_n = middle.n // 2
    add('gather_own', pltpu.VMEM((4 * (block_n // 4) * block_n, LANES), F32))
    add('gather_other', pltpu.VMEM((4 * (block_n // 4) * block_n, LANES), F32))
    add('gs', pltpu.SemaphoreType.DMA((3,)))
    add('gr', pltpu.SemaphoreType.DMA((3,)))
    add('ps', pltpu.SemaphoreType.DMA((4,)))
    add('pr', pltpu.SemaphoreType.DMA((4,)))
    add('load', pltpu.SemaphoreType.DMA((TILE,)))
    add('store', pltpu.SemaphoreType.DMA((edge,)))
    half = jax.ShapeDtypeStruct((edge * edge // 2, LANES), F32)
    return pl.pallas_call(
        functools.partial(kernel_body, names, edge),
        out_shape=(half, half),
        in_specs=[pl.BlockSpec(memory_space=pl.ANY)] * 2,
        out_specs=(pl.BlockSpec(memory_space=pl.ANY),) * 2,
        scratch_shapes=scratch,
        compiler_params=pltpu.CompilerParams(collective_id=0, has_side_effects=True, vmem_limit_bytes=66000000),
        name='multigrid',
    )(initial, source)


def unpack_body(red_ref, black_ref, out_ref):
    planes = red_ref.shape[0]
    first = pl.program_id(0) * planes + lax.axis_index('z') * (planes * pl.num_programs(0))
    even = lax.rem(lax.broadcasted_iota(jnp.int32, (LANES, LANES), 0) + lax.broadcasted_iota(jnp.int32, (LANES, LANES), 1), 2) == 0
    for k in range(planes):
        shift = lax.rem(2 * LANES - first - k, LANES)
        red, black = pltpu.roll(red_ref[k], shift, 1), pltpu.roll(black_ref[k], shift, 1)
        out_ref[2 * k] = jnp.where(even, red, black)
        out_ref[2 * k + 1] = jnp.where(even, black, red)


def unpack(red, black, edge):
    step = TILE
    spec = pl.BlockSpec((step, edge, LANES), lambda i: (i, 0, 0))
    return pl.pallas_call(
        unpack_body,
        grid=(edge // 2 // step,),
        out_shape=jax.ShapeDtypeStruct((edge, edge, LANES), F32),
        in_specs=[spec, spec],
        out_specs=pl.BlockSpec((2 * step, edge, LANES), lambda i: (i, 0, 0)),
        name='unpack',
    )(red.reshape(edge // 2, edge, LANES), black.reshape(edge // 2, edge, LANES))


def solution(mesh):
    grid_spec = P(('batch', 'z'), 'y', 'x')

    def local_solve(source, initial_guess):
        edge = source.shape[0]
        red, black = solve_packed(
            initial_guess.reshape(edge * edge, edge), source.reshape(edge * edge, edge), edge)
        return unpack(red, black, edge)

    return jax.shard_map(local_solve, mesh=mesh, in_specs=(grid_spec, grid_spec), out_specs=grid_spec, check_vma=False)
```

```python
import functools

import jax
import jax.numpy as jnp
from jax import lax
from jax.experimental import pallas as pl
from jax.experimental.pallas import tpu as pltpu
from jax.sharding import PartitionSpec as P

CYCLES = 2
COARSE_SWEEPS = 24
LANES = 128
WIDTH = 32
GROUP = 8
TILE = 8
MESH = pl.DeviceIdType.MESH
F32 = jnp.float32
SIXTH = 1.0 / 6.0
RED, BLACK = 0, 1
HIGHEST = lax.Precision.HIGHEST


def mult8(value):
    return value if isinstance(value, int) else pl.multiple_of(value, TILE)


def rows(start, size):
    return pl.ds(mult8(start), size)


class Level:
    def __init__(self, n, dist, width, unroll):
        self.n = n
        self.planes = n // 2
        self.nb = max(n, TILE)
        self.pitch = self.nb + 16
        self.dist = dist
        self.width = min(width, self.nb)
        self.chunks = self.nb // self.width
        self.unroll = min(unroll, self.planes)

    def scratch(self):
        cells = pltpu.VMEM(((self.planes + 2) * self.pitch, LANES), F32)
        packed = pltpu.VMEM((self.planes * self.nb, LANES), F32)
        shapes = dict(v0=cells, v1=cells, g0=packed, g1=packed)
        if self.dist:
            face_x = pltpu.VMEM((self.nb, LANES), F32)
            face_y = pltpu.VMEM((self.planes, LANES), F32)
            for colour in (RED, BLACK):
                shapes[f'fx{colour}'] = face_x
                shapes[f'hx{colour}'] = face_x
                shapes[f'fy{colour}'] = face_y
                shapes[f'hy{colour}'] = face_y
            for axis in ('x', 'z'):
                shapes[f's{axis}'] = pltpu.SemaphoreType.DMA((2 * self.chunks,))
                shapes[f'r{axis}'] = pltpu.SemaphoreType.DMA((2 * self.chunks,))
            shapes['sy'] = pltpu.SemaphoreType.DMA((2,))
            shapes['ry'] = pltpu.SemaphoreType.DMA((2,))
        return shapes

    def bind(self, refs):
        self.v = (refs['v0'], refs['v1'])
        self.g = (refs['g0'], refs['g1'])
        if self.dist:
            self.fx = (refs['fx0'], refs['fx1'])
            self.hx = (refs['hx0'], refs['hx1'])
            self.fy = (refs['fy0'], refs['fy1'])
            self.hy = (refs['hy0'], refs['hy1'])
            self.sems = {key: refs[key] for key in ('sx', 'rx', 'sz', 'rz', 'sy', 'ry')}


def make_levels(edge):
    levels = [Level(edge, True, WIDTH, 16), Level(edge // 2, True, WIDTH // 2, 16)]
    n = edge // 2
    while n >= 4:
        levels.append(Level(n, False, 2 * WIDTH, 16))
        n = n // 2
    return levels


def kernel_body(names, edge, *args):
    refs = dict(zip(names, args))
    xi, yi, zi = lax.axis_index('x'), lax.axis_index('y'), lax.axis_index('z')
    levels = make_levels(edge)
    for index, level in enumerate(levels):
        prefix = f'L{index}_'
        level.bind({key[len(prefix):]: ref for key, ref in refs.items() if key.startswith(prefix)})

    def lanes(size):
        return lax.broadcasted_iota(jnp.int32, (size, LANES), 1)

    def even_mask(size):
        return lax.rem(lanes(size) + lax.broadcasted_iota(jnp.int32, (size, LANES), 0), 2) == 0

    def side(level):
        return jnp.where(xi == 0, level.n - 1, 0)

    def turn(value, shift):
        return pltpu.roll(value, lax.rem(shift + 2 * LANES, LANES), 1)

    def skew(level, k):
        return k + level.planes * zi if level.dist else k

    def copy_x(level, colour, j):
        span = rows(j * level.width, level.width)
        k = colour * level.chunks + j
        return pltpu.make_async_remote_copy(
            src_ref=level.fx[colour].at[span], dst_ref=level.hx[colour].at[span],
            send_sem=level.sems['sx'].at[k], recv_sem=level.sems['rx'].at[k],
            device_id={'x': 1 - xi}, device_id_type=MESH)

    def copy_z(level, colour, j):
        offset = TILE + j * level.width
        src = jnp.where(zi == 0, level.planes, 1) * level.pitch + offset
        dst = jnp.where(zi == 0, 0, level.planes + 1) * level.pitch + offset
        k = colour * level.chunks + j
        return pltpu.make_async_remote_copy(
            src_ref=level.v[colour].at[rows(src, level.width)], dst_ref=level.v[colour].at[rows(dst, level.width)],
            send_sem=level.sems['sz'].at[k], recv_sem=level.sems['rz'].at[k],
            device_id={'z': 1 - zi}, device_id_type=MESH)

    def copy_y(level, colour):
        return pltpu.make_async_remote_copy(
            src_ref=level.fy[colour], dst_ref=level.hy[colour],
            send_sem=level.sems['sy'].at[colour], recv_sem=level.sems['ry'].at[colour],
            device_id={'y': 1 - yi}, device_id_type=MESH)

    def wait_y(level, colour):
        copy_y(level, colour).wait()
        ghost = jnp.where(yi == 0, level.n, -1)
        level.v[colour][pl.ds(level.pitch + TILE + ghost, level.planes, stride=level.pitch), :] = level.hy[colour][...]

    def wait_all(level, colour):
        wait_y(level, colour)

        def step(j, carry):
            copy_x(level, colour, j).wait()
            copy_z(level, colour, j).wait()
            return carry
        lax.fori_loop(0, level.chunks, step, 0)

    stage_u, stage_f = refs['stage_u'], refs['stage_f']

    def fill_ghosts(level, colour):
        own, other = level.v[colour], level.v[1 - colour]
        pitch, n = level.pitch, level.n

        def fill_row(src, dst):
            if level.planes >= TILE:
                values = own[pl.ds(pitch + TILE + src, level.planes, stride=pitch), :]
                other[pl.ds(pitch + TILE + dst, level.planes, stride=pitch), :] = -values
            else:
                for k in range(level.planes):
                    base = (k + 1) * pitch + TILE
                    other[pl.ds(base + dst, 1), :] = -own[pl.ds(base + src, 1), :]

        if level.dist:
            fill_row(jnp.where(yi == 0, 0, n - 1), jnp.where(yi == 0, -1, n))
        else:
            fill_row(0, -1)
            fill_row(n - 1, n)

    def half_sweep(level, colour, mode):
        own, other, source = level.v[colour], level.v[1 - colour], level.g[colour]
        width, pitch, n, planes = level.width, level.pitch, level.n, level.planes
        stencil = mode in ('gs', 'res0', 'res1')
        sends = level.dist and mode in ('gs', 'zero', 'copy')
        waits = level.dist and mode in ('gs', 'res0')
        if stencil:
            fill_ghosts(level, colour)
        if waits:
            wait_y(level, 1 - colour)
        lane = lanes(width)
        even = even_mask(width)
        odd = jnp.logical_not(even)
        takes_below = (even, odd) if colour == RED else (odd, even)
        q = side(level)

        def chunk(jj, carry):
            j = jnp.where(yi == 1, jj, level.chunks - 1 - jj) if level.dist else jj
            if waits:
                copy_x(level, 1 - colour, j).wait()
                copy_z(level, 1 - colour, j).wait()
            row0 = j * width + TILE
            blank = jnp.zeros((width, LANES), F32)
            unroll = level.unroll
            steps = planes // unroll
            pair_sum = refs['pair_sum']
            if stencil and level.dist:
                halo = level.hx[1 - colour][rows(j * width, width), :]

            reach = (unroll - 1) * pitch + width

            def block(ref, start):
                return ref[pl.ds(start, reach), :]

            def cut(values, start):
                return lax.slice(values, (start, 0), (start + width, LANES))

            def turned(here):
                return pltpu.roll(here, 1, 1), pltpu.roll(here, LANES - 1, 1)

            def ghost(plane, rotated, outside):
                return -plane if rotated is None else jnp.where(outside, -plane, rotated)

            def distance(place):
                return lax.bitwise_and(lane + (2 * LANES - place), LANES - 1)

            def along_x(old, u, place, face_place, left, right):
                ends = -old
                if level.dist:
                    ends = lax.select(face_place == u, halo, ends)
                left = lax.select(place == u, ends, left)
                return left + lax.select(place == (u + n - 1) % LANES, ends, right)

            def across(i, state):
                older, newer, sums = state
                start = mult8((i * unroll + 1) * pitch + row0)
                theirs = other[pl.ds(mult8(start + pitch), reach - pitch), :]
                mine = block(own, start)
                store = pair_sum.at[rows(i * (unroll * width), unroll * width)]
                place = distance(skew(level, i * unroll))
                face_place = distance(skew(level, i * unroll) + q)
                final = i == steps - 1
                old = cut(mine, 0)
                for u in range(unroll):
                    previous = old
                    if u < unroll - 1:
                        left, right = turned(cut(theirs, u * pitch))
                    else:
                        left, right = turned(other[rows(start + unroll * pitch, width), :])
                    if u < unroll - 1:
                        old = cut(mine, (u + 1) * pitch)
                    else:
                        outside = final & (zi == 1) if level.dist else final
                        right = ghost(previous, right, outside)
                        old = own[rows(start + jnp.where(final, u, unroll) * pitch, width), :]
                    sums = sums + lax.select(takes_below[u % 2], older, right)
                    store[u * width:(u + 1) * width, :] = sums
                    older, newer, sums = newer, left, along_x(old, u + 1, place, face_place, left, right)
                return older, newer, sums

            def update(i, face):
                start = mult8((i * unroll + 1) * pitch + row0)
                mine = own.at[pl.ds(start, reach)]
                packed = rows(i * (unroll * level.nb) + j * width, (unroll - 1) * level.nb + width)
                stage = stage_u.at[packed]
                face_place = distance(skew(level, i * unroll) + q)
                if mode != 'copy':
                    scaled = source[packed, :]
                if mode != 'zero' and mode != 'gs':
                    old = block(own, start)
                if stencil:
                    here, before, after = block(other, start), block(other, start - 1), block(other, start + 1)
                    across_sums = pair_sum[rows(i * (unroll * width), unroll * width), :]
                if mode == 'res1':
                    staged = stage[...]
                for u in range(unroll):
                    base, line = u * pitch, u * level.nb
                    if mode == 'copy':
                        new = cut(old, base)
                    elif mode == 'zero':
                        new = cut(scaled, line) * SIXTH
                    else:
                        total = cut(before, base) + cut(after, base) + cut(across_sums, u * width)
                        total = total + cut(here, base) + cut(scaled, line)
                        new = total * SIXTH if mode == 'gs' else total - 6.0 * cut(old, base)
                    if mode in ('gs', 'zero'):
                        mine[base:base + width, :] = new
                    elif mode == 'res0':
                        stage[line:line + width, :] = new
                    elif mode == 'res1':
                        stage[line:line + width, :] = cut(staged, line) + new
                    if sends:
                        face = lax.select(face_place == u, new, face)
                return face

            if stencil:
                first = own[rows(pitch + row0, width), :]
                below = turned(other[rows(row0, width), :])[0] if level.dist else None
                below = ghost(first, below, zi == 0)
                left, right = turned(other[rows(pitch + row0, width), :])
                place = skew(level, 0)
                state = across(0, (below, left, along_x(first, 0, distance(place), distance(place + q), left, right)))

                def planes_step(i, carried):
                    state, face = carried
                    state = across(i + 1, state)
                    return state, update(i, face)
                _, face = lax.fori_loop(0, steps - 1, planes_step, (state, blank))
                face = update(steps - 1, face)
            else:
                face = lax.fori_loop(0, steps, update, blank)
            if sends:
                level.fx[colour][rows(j * width, width), :] = turn(face, (2 * xi - 1) * (n - 1))
                copy_x(level, colour, j).start()
                copy_z(level, colour, j).start()

                @pl.when(jj == 0)
                def _():
                    y_row = jnp.where(yi == 0, n - 1, 0)
                    level.fy[colour][...] = own[pl.ds(pitch + TILE + y_row, planes, stride=pitch), :]
                    copy_y(level, colour).start()
            return carry

        lax.fori_loop(0, level.chunks, chunk, 0)

    def sweeps(level, count):
        def step(index, carry):
            half_sweep(level, RED, 'gs')
            half_sweep(level, BLACK, 'gs')
            return carry
        lax.fori_loop(0, count, step, 0)

    square_i = lax.broadcasted_iota(jnp.int32, (LANES, LANES), 0)
    square_f = lax.broadcasted_iota(jnp.int32, (LANES, LANES), 1)

    def restriction_matrix(n_coarse):
        hit = (lax.div(square_i, 2) == square_f) & (square_i < 2 * n_coarse)
        return jnp.where(hit, 0.5, 0.0).astype(F32)

    def prolongation_matrix(n_fine, n_coarse, offset, low_lane, high_lane):
        own_index = lax.div(square_f, 2) + offset
        near = jnp.where(lax.rem(square_f, 2) == 0, own_index - 1, own_index + 1)
        outside = (near < 0) | (near > n_coarse - 1)
        value = jnp.where(square_i == own_index, jnp.where(outside & (low_lane is None), 0.5, 0.75), 0.0)
        value = value + jnp.where((square_i == near) & jnp.logical_not(outside), 0.25, 0.0)
        return jnp.where(square_f < n_fine, value, 0.0).astype(F32)

    def distributed_matrix(n_coarse):
        own_index = lax.div(square_f, 2)
        near = jnp.where(lax.rem(square_f, 2) == 0, own_index - 1, own_index + 1)
        halo_near = jnp.where(xi == 0, n_coarse, -1)
        ghost_near = jnp.where(xi == 0, -1, n_coarse)
        lane_of_near = jnp.where(near == -1, 127, near)
        value = jnp.where(square_i == own_index, jnp.where(near == ghost_near, 0.5, 0.75), 0.0)
        inside = (near >= 0) & (near < n_coarse)
        value = value + jnp.where((square_i == lane_of_near) & (inside | (near == halo_near)), 0.25, 0.0)
        return value.astype(F32)

    def matmul(a, b):
        return jnp.dot(a, b, precision=HIGHEST, preferred_element_type=F32)

    def restrict_pair(level, k, matrix):
        n_coarse = level.n // 2
        size = max(n_coarse, TILE)
        pair = []
        for z in (0, 1):
            base = (2 * k + z) * level.nb
            total = stage_u[pl.ds(base, size, stride=2), :] + stage_u[pl.ds(base + 1, size, stride=2), :]
            pair.append(matmul(turn(total, -skew(level, 2 * k + z)), matrix))
        even = even_mask(size)
        return jnp.where(even, pair[0], pair[1]), jnp.where(even, pair[1], pair[0])

    def grouped(count, size, body):
        size = min(size, count)

        def step(i, carry):
            body([i * size + u for u in range(size)])
            return carry
        lax.fori_loop(0, count // size, step, 0)

    def restrict_local(level, coarse, index):
        matrix = refs[f'mat_q{index}'][...]

        def step(indices):
            pairs = [restrict_pair(level, k, matrix) for k in indices]
            pairs = [[turn(part, skew(coarse, k)) for part in pair] for k, pair in zip(indices, pairs)]
            for k, pair in zip(indices, pairs):
                for colour in (RED, BLACK):
                    coarse.g[colour][rows(k * coarse.nb, coarse.nb), :] = pair[colour]
        grouped(coarse.planes, GROUP, step)

    gather_own, gather_other = refs['gather_own'], refs['gather_other']
    fine_block = levels[1]
    block_n = fine_block.n // 2
    block_rows = (block_n // 4) * block_n
    slot = 2 * zi + yi

    def gather_copies():
        copies = []
        for index, flips in enumerate(((0, 1), (1, 0), (1, 1))):
            target = {'z': zi + flips[0] - 2 * zi * flips[0], 'y': yi + flips[1] - 2 * yi * flips[1]}
            here = gather_own.at[rows(slot * block_rows, block_rows)]
            copies.append(pltpu.make_async_remote_copy(
                src_ref=here, dst_ref=here, send_sem=refs['gs'].at[index], recv_sem=refs['gr'].at[index],
                device_id=target, device_id_type=MESH))
        return copies

    def partner_copy(index):
        flips = ((0, 0), (0, 1), (1, 0), (1, 1))[index]
        z = zi + flips[0] - 2 * zi * flips[0]
        y = yi + flips[1] - 2 * yi * flips[1]
        span = rows((2 * z + y) * block_rows, block_rows)
        return pltpu.make_async_remote_copy(
            src_ref=gather_own.at[span], dst_ref=gather_other.at[span],
            send_sem=refs['ps'].at[index], recv_sem=refs['pr'].at[index],
            device_id={'x': 1 - xi}, device_id_type=MESH)

    def restrict_gather(coarse):
        matrix = refs['mat_q1'][...]

        def step(indices):
            for m in indices:
                packed = None
                for half in (0, 1):
                    for colour, part in enumerate(restrict_pair(fine_block, 2 * m + half, matrix)):
                        part = turn(part, (2 * half + colour) * block_n)
                        packed = part if packed is None else packed + part
                gather_own[rows(slot * block_rows + m * block_n, block_n), :] = packed
        grouped(block_n // 4, GROUP, step)
        copies = gather_copies()
        for copy in copies:
            copy.start()
        partner_copy(0).start()
        for index, copy in enumerate(copies):
            copy.wait()
            partner_copy(index + 1).start()
        for index in range(4):
            partner_copy(index).wait()
        lane = lanes(block_n)

        def unpack_slot(source_slot, carry):
            zs, ys = lax.div(source_slot, 2), lax.rem(source_slot, 2)

            def unpack(indices):
                results = []
                for m in indices:
                    span = rows(source_slot * block_rows + m * block_n, block_n)
                    mine, theirs = gather_own[span, :], gather_other[span, :]
                    at_zero = jnp.where(xi == 0, mine, theirs)
                    at_one = jnp.where(xi == 0, theirs, mine)
                    for half in (0, 1):
                        plane = zs * (block_n // 2) + 2 * m + half
                        place = lax.bitwise_and(lane + (LANES - plane), LANES - 1)
                        low, middle = place < block_n, place < 2 * block_n
                        for colour in (RED, BLACK):
                            shift = plane - (2 * half + colour) * block_n
                            right = lax.select(middle, turn(at_one, shift + block_n), jnp.zeros_like(at_one))
                            results.append((colour, plane, lax.select(low, turn(at_zero, shift), right)))
                for colour, plane, value in results:
                    coarse.g[colour][rows(plane * coarse.nb + ys * block_n, block_n), :] = value
            grouped(block_n // 4, GROUP, unpack)
            return carry
        lax.fori_loop(0, 4, unpack_slot, 0)

    def set_zero(ref, size):
        def step(i, carry):
            ref[rows(i * TILE, TILE), :] = jnp.zeros((TILE, LANES), F32)
            return carry
        lax.fori_loop(0, size // TILE, step, 0)

    def expand_x(coarse, planes_ref, matrix):
        nb, pitch = coarse.nb, coarse.pitch
        lane = lanes(nb)
        even = even_mask(nb)
        keep = lane < coarse.n
        if coarse.dist:
            q = side(coarse)
            halo_lane = lane == jnp.where(xi == 0, coarse.n, 127)
            target_lane = jnp.where(xi == 0, coarse.n, 127)
            halos = [coarse.hx[colour][...] for colour in (RED, BLACK)]

        def step(indices):
            results = []
            for k in indices:
                parts = []
                for colour in (RED, BLACK):
                    value = turn(coarse.v[colour][rows((k + 1) * pitch + TILE, nb), :], -skew(coarse, k))
                    value = jnp.where(keep, value, 0.0)
                    if coarse.dist:
                        halo = turn(halos[colour], target_lane - q - skew(coarse, k))
                        value = jnp.where(halo_lane, halo, value)
                    parts.append(value)
                red, black = parts
                results.append(matmul(jnp.where(even, red, black), matrix))
                results.append(matmul(jnp.where(even, black, red), matrix))
            for offset, value in enumerate(results):
                planes_ref[rows((2 * indices[0] + 1 + offset) * pitch + TILE, nb), :] = value
        grouped(coarse.planes, GROUP, step)

    def negate_row(ref, src, dst):
        ref[pl.ds(dst, 1), :] = -ref[pl.ds(src, 1), :]

    def pad_local(coarse, planes_ref):
        n, pitch = coarse.n, coarse.pitch
        if n >= TILE:
            for src, dst in ((0, -1), (n - 1, n)):
                values = planes_ref[pl.ds(pitch + TILE + src, n, stride=pitch), :]
                planes_ref[pl.ds(pitch + TILE + dst, n, stride=pitch), :] = -values
        else:
            for k in range(1, n + 1):
                negate_row(planes_ref, k * pitch + TILE, k * pitch + 7)
                negate_row(planes_ref, k * pitch + TILE + n - 1, k * pitch + TILE + n)
        planes_ref[rows(0, pitch), :] = -planes_ref[rows(pitch, pitch), :]
        planes_ref[rows((n + 1) * pitch, pitch), :] = -planes_ref[rows(n * pitch, pitch), :]

    def pad_distributed(coarse, planes_ref):
        n, pitch = coarse.n, coarse.pitch
        y_own = jnp.where(yi == 0, n - 1, 0)
        y_halo = jnp.where(yi == 0, n, -1)
        z_own = jnp.where(zi == 0, n, 1)
        z_halo_mine = jnp.where(zi == 0, n + 1, 0)
        z_halo_theirs = jnp.where(zi == 0, 0, n + 1)
        refs['pfy'][...] = planes_ref[pl.ds(pitch + TILE + y_own, n, stride=pitch), :]
        copy_rows = pltpu.make_async_remote_copy(
            src_ref=refs['pfy'], dst_ref=refs['phy'], send_sem=refs['qs'].at[0], recv_sem=refs['qr'].at[0],
            device_id={'y': 1 - yi}, device_id_type=MESH)
        copy_plane = pltpu.make_async_remote_copy(
            src_ref=planes_ref.at[rows(z_own * pitch + TILE, n)], dst_ref=planes_ref.at[rows(z_halo_theirs * pitch + TILE, n)],
            send_sem=refs['qs'].at[1], recv_sem=refs['qr'].at[1],
            device_id={'z': 1 - zi}, device_id_type=MESH)
        corner = z_own * pitch + TILE + jnp.where(yi == 0, n - TILE, 0)
        copy_corner = pltpu.make_async_remote_copy(
            src_ref=planes_ref.at[rows(corner, TILE)], dst_ref=refs['phc'],
            send_sem=refs['qs'].at[2], recv_sem=refs['qr'].at[2],
            device_id={'z': 1 - zi, 'y': 1 - yi}, device_id_type=MESH)
        copy_rows.start()
        copy_plane.start()
        copy_corner.start()
        ghost_src, ghost_dst = jnp.where(yi == 0, 0, n - 1), jnp.where(yi == 0, -1, n)
        values = planes_ref[pl.ds(pitch + TILE + ghost_src, n, stride=pitch), :]
        planes_ref[pl.ds(pitch + TILE + ghost_dst, n, stride=pitch), :] = -values
        copy_rows.wait()
        planes_ref[pl.ds(pitch + TILE + y_halo, n, stride=pitch), :] = refs['phy'][...]
        copy_plane.wait()
        base = z_halo_mine * pitch + TILE
        negate_row(planes_ref, base + ghost_src, base + ghost_dst)
        copy_corner.wait()
        planes_ref[pl.ds(base + y_halo, 1), :] = refs['phc'][pl.ds(jnp.where(yi == 0, 0, 7), 1), :]
        z_edge, z_ghost = jnp.where(zi == 0, 1, n), jnp.where(zi == 0, 0, n + 1)
        planes_ref[rows(z_ghost * pitch, pitch), :] = -planes_ref[rows(z_edge * pitch, pitch), :]

    def expand_zy(coarse, planes_ref, fine, z_offset, y_offset):
        half = fine.n // 2
        size = half
        pitch = coarse.pitch
        even_lane = lax.rem(lanes(size), 2) == 0

        def step(indices):
            results = []
            for k in indices:
                middle = (k + z_offset + 1) * pitch + TILE + y_offset
                low, high = {}, {}
                for dy in (-1, 0, 1):
                    here = 0.75 * planes_ref[pl.ds(middle + dy, size), :]
                    low[dy] = here + 0.25 * planes_ref[pl.ds(middle - pitch + dy, size), :]
                    high[dy] = here + 0.25 * planes_ref[pl.ds(middle + pitch + dy, size), :]
                for odd in (0, 1):
                    dy = 2 * odd - 1
                    z_even = 0.75 * low[0] + 0.25 * low[dy]
                    z_odd = 0.75 * high[0] + 0.25 * high[dy]
                    first = turn(jnp.where(even_lane, z_even, z_odd), skew(fine, k))
                    second = turn(jnp.where(even_lane, z_odd, z_even), skew(fine, k))
                    span = pl.ds((k + 1) * fine.pitch + TILE + odd, size, stride=2)
                    for colour, change in ((odd, first), (1 - odd, second)):
                        results.append((colour, span, fine.v[colour][span, :] + change))
            for colour, span, value in results:
                fine.v[colour][span, :] = value
        grouped(fine.planes, 4, step)

    barrier = pltpu.get_barrier_semaphore()
    for target in ({'x': 1 - xi}, {'y': 1 - yi}, {'z': 1 - zi}, {'z': 1 - zi, 'y': 1 - yi}):
        pl.semaphore_signal(barrier, inc=1, device_id=target, device_id_type=MESH)
    pl.semaphore_wait(barrier, 4)

    top = levels[0]
    load_chunks = 4
    chunk_rows = edge * edge // load_chunks

    def load_copy(index, which):
        span = rows(index * chunk_rows, chunk_rows)
        return pltpu.make_async_copy(
            (refs['u_in'], refs['f_in'])[which].at[span], (stage_u, stage_f)[which].at[span],
            refs['load'].at[2 * index + which])

    for index in range(load_chunks):
        for which in (0, 1):
            load_copy(index, which).start()
    even_edge = even_mask(edge)
    scale = 1.0 / float((2 * edge) ** 2)

    def pack(index, carry):
        load_copy(index, 0).wait()
        load_copy(index, 1).wait()

        per_chunk = top.planes // load_chunks

        def step(indices):
            for i in indices:
                k = index * per_chunk + i
                for stage, target, start in ((stage_u, top.v, (k + 1) * top.pitch + TILE), (stage_f, top.g, k * edge)):
                    a, b = stage[rows(2 * k * edge, edge), :], stage[rows((2 * k + 1) * edge, edge), :]
                    if stage is stage_f:
                        a, b = a * scale, b * scale
                    target[RED][rows(start, edge), :] = turn(jnp.where(even_edge, a, b), skew(top, k))
                    target[BLACK][rows(start, edge), :] = turn(jnp.where(even_edge, b, a), skew(top, k))
        grouped(per_chunk, 2, step)
        return carry
    lax.fori_loop(0, load_chunks, pack, 0)

    for index in range(len(levels) - 1):
        refs[f'mat_q{index}'][...] = restriction_matrix(levels[index].n // 2)
    refs['mat_p0'][...] = distributed_matrix(levels[1].n)
    refs['mat_p1'][...] = prolongation_matrix(levels[1].n, levels[2].n, xi * (levels[2].n // 2), None, None)
    for index in range(2, len(levels) - 1):
        fine_n = levels[index].n
        refs[f'mat_p{index}'][...] = prolongation_matrix(fine_n, fine_n // 2, 0, None, None)

    planes_dist, planes_local = refs['planes_dist'], refs['planes_local']

    def residual(level):
        half_sweep(level, RED, 'res0')
        half_sweep(level, BLACK, 'res1')

    def solve(level, sweep_count, phases, descend):
        def phase(p, carry):
            def sweep(index, inner):
                fresh = (p == 0) & (index == 0)

                @pl.when(fresh)
                def _():
                    set_zero(level.v[BLACK], (level.planes + 2) * level.pitch)
                    half_sweep(level, RED, 'zero')

                @pl.when(jnp.logical_not(fresh))
                def _():
                    half_sweep(level, RED, 'gs')
                half_sweep(level, BLACK, 'gs')
                return inner
            lax.fori_loop(0, sweep_count, sweep, 0)
            if phases == 2:
                @pl.when(p == 0)
                def _():
                    residual(level)
                    descend()
            return carry
        lax.fori_loop(0, phases, phase, 0)

    def solve_local(index):
        level = levels[index]
        if index == len(levels) - 1:
            solve(level, COARSE_SWEEPS, 1, None)
            return

        def descend():
            restrict_local(level, levels[index + 1], index)
            solve_local(index + 1)
            expand_x(levels[index + 1], planes_local, refs[f'mat_p{index}'][...])
            pad_local(levels[index + 1], planes_local)
            expand_zy(levels[index + 1], planes_local, level, 0, 0)
        solve(level, 2, 2, descend)

    middle, replicated = levels[1], levels[2]

    def descend_middle():
        restrict_gather(replicated)
        solve_local(2)
        expand_x(replicated, planes_local, refs['mat_p1'][...])
        pad_local(replicated, planes_local)
        expand_zy(replicated, planes_local, middle, zi * (replicated.n // 2), yi * (replicated.n // 2))
        half_sweep(middle, BLACK, 'copy')

    half_sweep(top, BLACK, 'copy')

    def sweep_pair(index, carry):
        sweeps(top, 2)

        @pl.when(lax.rem(index, 2) == 0)
        def _():
            residual(top)
            restrict_local(top, middle, 0)
            solve(middle, 2, 2, descend_middle)
            wait_all(middle, BLACK)
            expand_x(middle, planes_dist, refs['mat_p0'][...])
            pad_distributed(middle, planes_dist)
            expand_zy(middle, planes_dist, top, 0, 0)
            half_sweep(top, BLACK, 'copy')
        return carry
    lax.fori_loop(0, 2 * CYCLES, sweep_pair, 0)
    wait_all(top, BLACK)

    def store_copy(k, colour):
        return pltpu.make_async_copy(
            top.v[colour].at[rows((k + 1) * top.pitch + TILE, edge)],
            (refs['red_out'], refs['black_out'])[colour].at[rows(k * edge, edge)], refs['store'].at[2 * k + colour])

    def store_start(k, carry):
        store_copy(k, RED).start()
        store_copy(k, BLACK).start()
        return carry

    def store_wait(k, carry):
        store_copy(k, RED).wait()
        store_copy(k, BLACK).wait()
        return carry
    lax.fori_loop(0, top.planes, store_start, 0)
    lax.fori_loop(0, top.planes, store_wait, 0)


def solve_packed(initial, source, edge):
    levels = make_levels(edge)
    names = ['u_in', 'f_in', 'red_out', 'black_out']
    scratch = []

    def add(name, shape):
        names.append(name)
        scratch.append(shape)

    for index, level in enumerate(levels):
        for key, shape in level.scratch().items():
            add(f'L{index}_{key}', shape)
    add('stage_u', pltpu.VMEM((edge * edge, LANES), F32))
    add('stage_f', pltpu.VMEM((edge * edge, LANES), F32))
    add('pair_sum', pltpu.VMEM((edge * WIDTH, LANES), F32))
    for index in range(len(levels) - 1):
        add(f'mat_p{index}', pltpu.VMEM((LANES, LANES), F32))
        add(f'mat_q{index}', pltpu.VMEM((LANES, LANES), F32))
    middle, replicated = levels[1], levels[2]
    add('planes_dist', pltpu.VMEM(((middle.n + 2) * middle.pitch, LANES), F32))
    add('planes_local', pltpu.VMEM(((replicated.n + 2) * replicated.pitch, LANES), F32))
    add('pfy', pltpu.VMEM((middle.n, LANES), F32))
    add('phy', pltpu.VMEM((middle.n, LANES), F32))
    add('phc', pltpu.VMEM((TILE, LANES), F32))
    add('qs', pltpu.SemaphoreType.DMA((3,)))
    add('qr', pltpu.SemaphoreType.DMA((3,)))
    block_n = middle.n // 2
    add('gather_own', pltpu.VMEM((4 * (block_n // 4) * block_n, LANES), F32))
    add('gather_other', pltpu.VMEM((4 * (block_n // 4) * block_n, LANES), F32))
    add('gs', pltpu.SemaphoreType.DMA((3,)))
    add('gr', pltpu.SemaphoreType.DMA((3,)))
    add('ps', pltpu.SemaphoreType.DMA((4,)))
    add('pr', pltpu.SemaphoreType.DMA((4,)))
    add('load', pltpu.SemaphoreType.DMA((TILE,)))
    add('store', pltpu.SemaphoreType.DMA((edge,)))
    half = jax.ShapeDtypeStruct((edge * edge // 2, LANES), F32)
    return pl.pallas_call(
        functools.partial(kernel_body, names, edge),
        out_shape=(half, half),
        in_specs=[pl.BlockSpec(memory_space=pl.ANY)] * 2,
        out_specs=(pl.BlockSpec(memory_space=pl.ANY),) * 2,
        scratch_shapes=scratch,
        compiler_params=pltpu.CompilerParams(collective_id=0, has_side_effects=True, vmem_limit_bytes=66000000),
        name='multigrid',
    )(initial, source)


def unpack_body(red_ref, black_ref, out_ref):
    planes = red_ref.shape[0]
    first = pl.program_id(0) * planes + lax.axis_index('z') * (planes * pl.num_programs(0))
    even = lax.rem(lax.broadcasted_iota(jnp.int32, (LANES, LANES), 0) + lax.broadcasted_iota(jnp.int32, (LANES, LANES), 1), 2) == 0
    for k in range(planes):
        shift = lax.rem(2 * LANES - first - k, LANES)
        red, black = pltpu.roll(red_ref[k], shift, 1), pltpu.roll(black_ref[k], shift, 1)
        out_ref[2 * k] = jnp.where(even, red, black)
        out_ref[2 * k + 1] = jnp.where(even, black, red)


def unpack(red, black, edge):
    step = TILE
    spec = pl.BlockSpec((step, edge, LANES), lambda i: (i, 0, 0))
    return pl.pallas_call(
        unpack_body,
        grid=(edge // 2 // step,),
        out_shape=jax.ShapeDtypeStruct((edge, edge, LANES), F32),
        in_specs=[spec, spec],
        out_specs=pl.BlockSpec((2 * step, edge, LANES), lambda i: (i, 0, 0)),
        name='unpack',
    )(red.reshape(edge // 2, edge, LANES), black.reshape(edge // 2, edge, LANES))


def solution(mesh):
    grid_spec = P(('batch', 'z'), 'y', 'x')

    def local_solve(source, initial_guess):
        edge = source.shape[0]
        red, black = solve_packed(
            initial_guess.reshape(edge * edge, edge), source.reshape(edge * edge, edge), edge)
        return unpack(red, black, edge)

    return jax.shard_map(local_solve, mesh=mesh, in_specs=(grid_spec, grid_spec), out_specs=grid_spec, check_vma=False)
```

```python
import functools

import jax
import jax.numpy as jnp
from jax import lax
from jax.experimental import pallas as pl
from jax.experimental.pallas import tpu as pltpu
from jax.sharding import PartitionSpec as P

CYCLES = 2
COARSE_SWEEPS = 24
LANES = 128
WIDTH = 32
GROUP = 8
TILE = 8
MESH = pl.DeviceIdType.MESH
F32 = jnp.float32
SIXTH = 1.0 / 6.0
RED, BLACK = 0, 1
HIGHEST = lax.Precision.HIGHEST


def mult8(value):
    return value if isinstance(value, int) else pl.multiple_of(value, TILE)


def rows(start, size):
    return pl.ds(mult8(start), size)


class Level:
    def __init__(self, n, dist, width, unroll):
        self.n = n
        self.planes = n // 2
        self.nb = max(n, TILE)
        self.pitch = self.nb + 16
        self.dist = dist
        self.width = min(width, self.nb)
        self.chunks = self.nb // self.width
        self.unroll = min(unroll, self.planes)

    def scratch(self):
        cells = pltpu.VMEM(((self.planes + 2) * self.pitch, LANES), F32)
        packed = pltpu.VMEM((self.planes * self.nb, LANES), F32)
        shapes = dict(v0=cells, v1=cells, g0=packed, g1=packed)
        if self.dist:
            face_x = pltpu.VMEM((self.nb, LANES), F32)
            face_y = pltpu.VMEM((self.planes, LANES), F32)
            for colour in (RED, BLACK):
                shapes[f'fx{colour}'] = face_x
                shapes[f'hx{colour}'] = face_x
                shapes[f'fy{colour}'] = face_y
                shapes[f'hy{colour}'] = face_y
            for axis in ('x', 'z'):
                shapes[f's{axis}'] = pltpu.SemaphoreType.DMA((2 * self.chunks,))
                shapes[f'r{axis}'] = pltpu.SemaphoreType.DMA((2 * self.chunks,))
            shapes['sy'] = pltpu.SemaphoreType.DMA((2,))
            shapes['ry'] = pltpu.SemaphoreType.DMA((2,))
        return shapes

    def bind(self, refs):
        self.v = (refs['v0'], refs['v1'])
        self.g = (refs['g0'], refs['g1'])
        if self.dist:
            self.fx = (refs['fx0'], refs['fx1'])
            self.hx = (refs['hx0'], refs['hx1'])
            self.fy = (refs['fy0'], refs['fy1'])
            self.hy = (refs['hy0'], refs['hy1'])
            self.sems = {key: refs[key] for key in ('sx', 'rx', 'sz', 'rz', 'sy', 'ry')}


def make_levels(edge):
    levels = [Level(edge, True, WIDTH, 16), Level(edge // 2, True, WIDTH // 2, 16)]
    n = edge // 2
    while n >= 4:
        levels.append(Level(n, False, 2 * WIDTH, 16))
        n = n // 2
    return levels


def kernel_body(names, edge, *args):
    refs = dict(zip(names, args))
    xi, yi, zi = lax.axis_index('x'), lax.axis_index('y'), lax.axis_index('z')
    levels = make_levels(edge)
    for index, level in enumerate(levels):
        prefix = f'L{index}_'
        level.bind({key[len(prefix):]: ref for key, ref in refs.items() if key.startswith(prefix)})

    def lanes(size):
        return lax.broadcasted_iota(jnp.int32, (size, LANES), 1)

    def even_mask(size):
        return lax.rem(lanes(size) + lax.broadcasted_iota(jnp.int32, (size, LANES), 0), 2) == 0

    def side(level):
        return jnp.where(xi == 0, level.n - 1, 0)

    def turn(value, shift):
        return pltpu.roll(value, lax.rem(shift + 2 * LANES, LANES), 1)

    def skew(level, k):
        return k + level.planes * zi if level.dist else k

    def copy_x(level, colour, j):
        span = rows(j * level.width, level.width)
        k = colour * level.chunks + j
        return pltpu.make_async_remote_copy(
            src_ref=level.fx[colour].at[span], dst_ref=level.hx[colour].at[span],
            send_sem=level.sems['sx'].at[k], recv_sem=level.sems['rx'].at[k],
            device_id={'x': 1 - xi}, device_id_type=MESH)

    def copy_z(level, colour, j):
        offset = TILE + j * level.width
        src = jnp.where(zi == 0, level.planes, 1) * level.pitch + offset
        dst = jnp.where(zi == 0, 0, level.planes + 1) * level.pitch + offset
        k = colour * level.chunks + j
        return pltpu.make_async_remote_copy(
            src_ref=level.v[colour].at[rows(src, level.width)], dst_ref=level.v[colour].at[rows(dst, level.width)],
            send_sem=level.sems['sz'].at[k], recv_sem=level.sems['rz'].at[k],
            device_id={'z': 1 - zi}, device_id_type=MESH)

    def copy_y(level, colour):
        return pltpu.make_async_remote_copy(
            src_ref=level.fy[colour], dst_ref=level.hy[colour],
            send_sem=level.sems['sy'].at[colour], recv_sem=level.sems['ry'].at[colour],
            device_id={'y': 1 - yi}, device_id_type=MESH)

    def wait_y(level, colour):
        copy_y(level, colour).wait()
        ghost = jnp.where(yi == 0, level.n, -1)
        level.v[colour][pl.ds(level.pitch + TILE + ghost, level.planes, stride=level.pitch), :] = level.hy[colour][...]

    def wait_all(level, colour):
        wait_y(level, colour)

        def step(j, carry):
            copy_x(level, colour, j).wait()
            copy_z(level, colour, j).wait()
            return carry
        lax.fori_loop(0, level.chunks, step, 0)

    stage_u, stage_f = refs['stage_u'], refs['stage_f']

    def fill_ghosts(level, colour):
        own, other = level.v[colour], level.v[1 - colour]
        pitch, n = level.pitch, level.n

        def fill_row(src, dst):
            if level.planes >= TILE:
                values = own[pl.ds(pitch + TILE + src, level.planes, stride=pitch), :]
                other[pl.ds(pitch + TILE + dst, level.planes, stride=pitch), :] = -values
            else:
                for k in range(level.planes):
                    base = (k + 1) * pitch + TILE
                    other[pl.ds(base + dst, 1), :] = -own[pl.ds(base + src, 1), :]

        if level.dist:
            fill_row(jnp.where(yi == 0, 0, n - 1), jnp.where(yi == 0, -1, n))
        else:
            fill_row(0, -1)
            fill_row(n - 1, n)

    def half_sweep(level, colour, mode):
        own, other, source = level.v[colour], level.v[1 - colour], level.g[colour]
        width, pitch, n, planes = level.width, level.pitch, level.n, level.planes
        stencil = mode in ('gs', 'res0', 'res1')
        sends = level.dist and mode in ('gs', 'zero', 'copy')
        waits = level.dist and mode in ('gs', 'res0')
        if stencil:
            fill_ghosts(level, colour)
        if waits:
            wait_y(level, 1 - colour)
        lane = lanes(width)
        even = even_mask(width)
        odd = jnp.logical_not(even)
        takes_below = (even, odd) if colour == RED else (odd, even)
        q = side(level)

        def chunk(jj, carry):
            j = jnp.where(yi == 1, jj, level.chunks - 1 - jj) if level.dist else jj
            if waits:
                copy_x(level, 1 - colour, j).wait()
                copy_z(level, 1 - colour, j).wait()
            row0 = j * width + TILE
            blank = jnp.zeros((width, LANES), F32)
            unroll = level.unroll
            steps = planes // unroll
            pair_sum = refs['pair_sum']
            if stencil and level.dist:
                halo = level.hx[1 - colour][rows(j * width, width), :]

            reach = (unroll - 1) * pitch + width

            def block(ref, start):
                return ref[pl.ds(start, reach), :]

            def cut(values, start):
                return lax.slice(values, (start, 0), (start + width, LANES))

            def turned(here):
                return pltpu.roll(here, 1, 1), pltpu.roll(here, LANES - 1, 1)

            def ghost(plane, rotated, outside):
                return -plane if rotated is None else jnp.where(outside, -plane, rotated)

            def distance(place):
                return lax.bitwise_and(lane + (2 * LANES - place), LANES - 1)

            def along_x(old, u, place, face_place, left, right):
                ends = -old
                if level.dist:
                    ends = lax.select(face_place == u, halo, ends)
                left = lax.select(place == u, ends, left)
                return left + lax.select(place == (u + n - 1) % LANES, ends, right)

            def across(i, state):
                older, newer, sums = state
                start = mult8((i * unroll + 1) * pitch + row0)
                theirs = other[pl.ds(mult8(start + pitch), reach - pitch), :]
                mine = block(own, start)
                store = pair_sum.at[rows(i * (unroll * width), unroll * width)]
                place = distance(skew(level, i * unroll))
                face_place = distance(skew(level, i * unroll) + q)
                final = i == steps - 1
                old = cut(mine, 0)
                for u in range(unroll):
                    previous = old
                    if u < unroll - 1:
                        left, right = turned(cut(theirs, u * pitch))
                    else:
                        left, right = turned(other[rows(start + unroll * pitch, width), :])
                    if u < unroll - 1:
                        old = cut(mine, (u + 1) * pitch)
                    else:
                        outside = final & (zi == 1) if level.dist else final
                        right = ghost(previous, right, outside)
                        old = own[rows(start + jnp.where(final, u, unroll) * pitch, width), :]
                    sums = sums + lax.select(takes_below[u % 2], older, right)
                    store[u * width:(u + 1) * width, :] = sums
                    older, newer, sums = newer, left, along_x(old, u + 1, place, face_place, left, right)
                return older, newer, sums

            def update(i, face):
                start = mult8((i * unroll + 1) * pitch + row0)
                mine = own.at[pl.ds(start, reach)]
                packed = rows(i * (unroll * level.nb) + j * width, (unroll - 1) * level.nb + width)
                stage = stage_u.at[packed]
                face_place = distance(skew(level, i * unroll) + q)
                if mode != 'copy':
                    scaled = source[packed, :]
                if mode != 'zero' and mode != 'gs':
                    old = block(own, start)
                if stencil:
                    here, before, after = block(other, start), block(other, start - 1), block(other, start + 1)
                    across_sums = pair_sum[rows(i * (unroll * width), unroll * width), :]
                if mode == 'res1':
                    staged = stage[...]
                for u in range(unroll):
                    base, line = u * pitch, u * level.nb
                    if mode == 'copy':
                        new = cut(old, base)
                    elif mode == 'zero':
                        new = cut(scaled, line) * SIXTH
                    else:
                        total = cut(before, base) + cut(after, base) + cut(across_sums, u * width)
                        total = total + cut(here, base) + cut(scaled, line)
                        new = total * SIXTH if mode == 'gs' else total - 6.0 * cut(old, base)
                    if mode in ('gs', 'zero'):
                        mine[base:base + width, :] = new
                    elif mode == 'res0':
                        stage[line:line + width, :] = new
                    elif mode == 'res1':
                        stage[line:line + width, :] = cut(staged, line) + new
                    if sends:
                        face = lax.select(face_place == u, new, face)
                return face

            if stencil:
                first = own[rows(pitch + row0, width), :]
                below = turned(other[rows(row0, width), :])[0] if level.dist else None
                below = ghost(first, below, zi == 0)
                left, right = turned(other[rows(pitch + row0, width), :])
                place = skew(level, 0)
                state = across(0, (below, left, along_x(first, 0, distance(place), distance(place + q), left, right)))

                def planes_step(i, carried):
                    state, face = carried
                    state = across(i + 1, state)
                    return state, update(i, face)
                _, face = lax.fori_loop(0, steps - 1, planes_step, (state, blank))
                face = update(steps - 1, face)
            else:
                face = lax.fori_loop(0, steps, update, blank)
            if sends:
                level.fx[colour][rows(j * width, width), :] = turn(face, (2 * xi - 1) * (n - 1))
                copy_x(level, colour, j).start()
                copy_z(level, colour, j).start()

                @pl.when(jj == 0)
                def _():
                    y_row = jnp.where(yi == 0, n - 1, 0)
                    level.fy[colour][...] = own[pl.ds(pitch + TILE + y_row, planes, stride=pitch), :]
                    copy_y(level, colour).start()
            return carry

        lax.fori_loop(0, level.chunks, chunk, 0)

    def sweeps(level, count):
        def step(index, carry):
            half_sweep(level, RED, 'gs')
            half_sweep(level, BLACK, 'gs')
            return carry
        lax.fori_loop(0, count, step, 0)

    square_i = lax.broadcasted_iota(jnp.int32, (LANES, LANES), 0)
    square_f = lax.broadcasted_iota(jnp.int32, (LANES, LANES), 1)

    def restriction_matrix(n_coarse):
        hit = (lax.div(square_i, 2) == square_f) & (square_i < 2 * n_coarse)
        return jnp.where(hit, 0.5, 0.0).astype(F32)

    def prolongation_matrix(n_fine, n_coarse, offset, low_lane, high_lane):
        own_index = lax.div(square_f, 2) + offset
        near = jnp.where(lax.rem(square_f, 2) == 0, own_index - 1, own_index + 1)
        outside = (near < 0) | (near > n_coarse - 1)
        value = jnp.where(square_i == own_index, jnp.where(outside & (low_lane is None), 0.5, 0.75), 0.0)
        value = value + jnp.where((square_i == near) & jnp.logical_not(outside), 0.25, 0.0)
        return jnp.where(square_f < n_fine, value, 0.0).astype(F32)

    def distributed_matrix(n_coarse):
        own_index = lax.div(square_f, 2)
        near = jnp.where(lax.rem(square_f, 2) == 0, own_index - 1, own_index + 1)
        halo_near = jnp.where(xi == 0, n_coarse, -1)
        ghost_near = jnp.where(xi == 0, -1, n_coarse)
        lane_of_near = jnp.where(near == -1, 127, near)
        value = jnp.where(square_i == own_index, jnp.where(near == ghost_near, 0.5, 0.75), 0.0)
        inside = (near >= 0) & (near < n_coarse)
        value = value + jnp.where((square_i == lane_of_near) & (inside | (near == halo_near)), 0.25, 0.0)
        return value.astype(F32)

    def matmul(a, b):
        return jnp.dot(a, b, precision=HIGHEST, preferred_element_type=F32)

    def restrict_pair(level, k, matrix):
        n_coarse = level.n // 2
        size = max(n_coarse, TILE)
        pair = []
        for z in (0, 1):
            base = (2 * k + z) * level.nb
            total = stage_u[pl.ds(base, size, stride=2), :] + stage_u[pl.ds(base + 1, size, stride=2), :]
            pair.append(matmul(turn(total, -skew(level, 2 * k + z)), matrix))
        even = even_mask(size)
        return jnp.where(even, pair[0], pair[1]), jnp.where(even, pair[1], pair[0])

    def grouped(count, size, body):
        size = min(size, count)

        def step(i, carry):
            body([i * size + u for u in range(size)])
            return carry
        lax.fori_loop(0, count // size, step, 0)

    def restrict_local(level, coarse, index):
        matrix = refs[f'mat_q{index}'][...]

        def step(indices):
            pairs = [restrict_pair(level, k, matrix) for k in indices]
            pairs = [[turn(part, skew(coarse, k)) for part in pair] for k, pair in zip(indices, pairs)]
            for k, pair in zip(indices, pairs):
                for colour in (RED, BLACK):
                    coarse.g[colour][rows(k * coarse.nb, coarse.nb), :] = pair[colour]
        grouped(coarse.planes, GROUP, step)

    gather_own, gather_other = refs['gather_own'], refs['gather_other']
    fine_block = levels[1]
    block_n = fine_block.n // 2
    block_rows = (block_n // 4) * block_n
    slot = 2 * zi + yi

    def gather_copies():
        copies = []
        for index, flips in enumerate(((0, 1), (1, 0), (1, 1))):
            target = {'z': zi + flips[0] - 2 * zi * flips[0], 'y': yi + flips[1] - 2 * yi * flips[1]}
            here = gather_own.at[rows(slot * block_rows, block_rows)]
            copies.append(pltpu.make_async_remote_copy(
                src_ref=here, dst_ref=here, send_sem=refs['gs'].at[index], recv_sem=refs['gr'].at[index],
                device_id=target, device_id_type=MESH))
        return copies

    def partner_copy(index):
        flips = ((0, 0), (0, 1), (1, 0), (1, 1))[index]
        z = zi + flips[0] - 2 * zi * flips[0]
        y = yi + flips[1] - 2 * yi * flips[1]
        span = rows((2 * z + y) * block_rows, block_rows)
        return pltpu.make_async_remote_copy(
            src_ref=gather_own.at[span], dst_ref=gather_other.at[span],
            send_sem=refs['ps'].at[index], recv_sem=refs['pr'].at[index],
            device_id={'x': 1 - xi}, device_id_type=MESH)

    def restrict_gather(coarse):
        matrix = refs['mat_q1'][...]

        def step(indices):
            for m in indices:
                packed = None
                for half in (0, 1):
                    for colour, part in enumerate(restrict_pair(fine_block, 2 * m + half, matrix)):
                        part = turn(part, (2 * half + colour) * block_n)
                        packed = part if packed is None else packed + part
                gather_own[rows(slot * block_rows + m * block_n, block_n), :] = packed
        grouped(block_n // 4, GROUP, step)
        copies = gather_copies()
        for copy in copies:
            copy.start()
        partner_copy(0).start()
        for index, copy in enumerate(copies):
            copy.wait()
            partner_copy(index + 1).start()
        for index in range(4):
            partner_copy(index).wait()
        lane = lanes(block_n)

        def unpack_slot(source_slot, carry):
            zs, ys = lax.div(source_slot, 2), lax.rem(source_slot, 2)

            def unpack(indices):
                results = []
                for m in indices:
                    span = rows(source_slot * block_rows + m * block_n, block_n)
                    mine, theirs = gather_own[span, :], gather_other[span, :]
                    at_zero = jnp.where(xi == 0, mine, theirs)
                    at_one = jnp.where(xi == 0, theirs, mine)
                    for half in (0, 1):
                        plane = zs * (block_n // 2) + 2 * m + half
                        place = lax.bitwise_and(lane + (LANES - plane), LANES - 1)
                        low, middle = place < block_n, place < 2 * block_n
                        for colour in (RED, BLACK):
                            shift = plane - (2 * half + colour) * block_n
                            right = lax.select(middle, turn(at_one, shift + block_n), jnp.zeros_like(at_one))
                            results.append((colour, plane, lax.select(low, turn(at_zero, shift), right)))
                for colour, plane, value in results:
                    coarse.g[colour][rows(plane * coarse.nb + ys * block_n, block_n), :] = value
            grouped(block_n // 4, GROUP, unpack)
            return carry
        lax.fori_loop(0, 4, unpack_slot, 0)

    def set_zero(ref, size):
        def step(i, carry):
            ref[rows(i * TILE, TILE), :] = jnp.zeros((TILE, LANES), F32)
            return carry
        lax.fori_loop(0, size // TILE, step, 0)

    def expand_x(coarse, planes_ref, matrix):
        nb, pitch = coarse.nb, coarse.pitch
        lane = lanes(nb)
        even = even_mask(nb)
        keep = lane < coarse.n
        if coarse.dist:
            q = side(coarse)
            halo_lane = lane == jnp.where(xi == 0, coarse.n, 127)
            target_lane = jnp.where(xi == 0, coarse.n, 127)
            halos = [coarse.hx[colour][...] for colour in (RED, BLACK)]

        def step(indices):
            results = []
            for k in indices:
                parts = []
                for colour in (RED, BLACK):
                    value = turn(coarse.v[colour][rows((k + 1) * pitch + TILE, nb), :], -skew(coarse, k))
                    value = jnp.where(keep, value, 0.0)
                    if coarse.dist:
                        halo = turn(halos[colour], target_lane - q - skew(coarse, k))
                        value = jnp.where(halo_lane, halo, value)
                    parts.append(value)
                red, black = parts
                results.append(matmul(jnp.where(even, red, black), matrix))
                results.append(matmul(jnp.where(even, black, red), matrix))
            for offset, value in enumerate(results):
                planes_ref[rows((2 * indices[0] + 1 + offset) * pitch + TILE, nb), :] = value
        grouped(coarse.planes, GROUP, step)

    def negate_row(ref, src, dst):
        ref[pl.ds(dst, 1), :] = -ref[pl.ds(src, 1), :]

    def pad_local(coarse, planes_ref):
        n, pitch = coarse.n, coarse.pitch
        if n >= TILE:
            for src, dst in ((0, -1), (n - 1, n)):
                values = planes_ref[pl.ds(pitch + TILE + src, n, stride=pitch), :]
                planes_ref[pl.ds(pitch + TILE + dst, n, stride=pitch), :] = -values
        else:
            for k in range(1, n + 1):
                negate_row(planes_ref, k * pitch + TILE, k * pitch + 7)
                negate_row(planes_ref, k * pitch + TILE + n - 1, k * pitch + TILE + n)
        planes_ref[rows(0, pitch), :] = -planes_ref[rows(pitch, pitch), :]
        planes_ref[rows((n + 1) * pitch, pitch), :] = -planes_ref[rows(n * pitch, pitch), :]

    def pad_distributed(coarse, planes_ref):
        n, pitch = coarse.n, coarse.pitch
        y_own = jnp.where(yi == 0, n - 1, 0)
        y_halo = jnp.where(yi == 0, n, -1)
        z_own = jnp.where(zi == 0, n, 1)
        z_halo_mine = jnp.where(zi == 0, n + 1, 0)
        z_halo_theirs = jnp.where(zi == 0, 0, n + 1)
        refs['pfy'][...] = planes_ref[pl.ds(pitch + TILE + y_own, n, stride=pitch), :]
        copy_rows = pltpu.make_async_remote_copy(
            src_ref=refs['pfy'], dst_ref=refs['phy'], send_sem=refs['qs'].at[0], recv_sem=refs['qr'].at[0],
            device_id={'y': 1 - yi}, device_id_type=MESH)
        copy_plane = pltpu.make_async_remote_copy(
            src_ref=planes_ref.at[rows(z_own * pitch + TILE, n)], dst_ref=planes_ref.at[rows(z_halo_theirs * pitch + TILE, n)],
            send_sem=refs['qs'].at[1], recv_sem=refs['qr'].at[1],
            device_id={'z': 1 - zi}, device_id_type=MESH)
        corner = z_own * pitch + TILE + jnp.where(yi == 0, n - TILE, 0)
        copy_corner = pltpu.make_async_remote_copy(
            src_ref=planes_ref.at[rows(corner, TILE)], dst_ref=refs['phc'],
            send_sem=refs['qs'].at[2], recv_sem=refs['qr'].at[2],
            device_id={'z': 1 - zi, 'y': 1 - yi}, device_id_type=MESH)
        copy_rows.start()
        copy_plane.start()
        copy_corner.start()
        ghost_src, ghost_dst = jnp.where(yi == 0, 0, n - 1), jnp.where(yi == 0, -1, n)
        values = planes_ref[pl.ds(pitch + TILE + ghost_src, n, stride=pitch), :]
        planes_ref[pl.ds(pitch + TILE + ghost_dst, n, stride=pitch), :] = -values
        copy_rows.wait()
        planes_ref[pl.ds(pitch + TILE + y_halo, n, stride=pitch), :] = refs['phy'][...]
        copy_plane.wait()
        base = z_halo_mine * pitch + TILE
        negate_row(planes_ref, base + ghost_src, base + ghost_dst)
        copy_corner.wait()
        planes_ref[pl.ds(base + y_halo, 1), :] = refs['phc'][pl.ds(jnp.where(yi == 0, 0, 7), 1), :]
        z_edge, z_ghost = jnp.where(zi == 0, 1, n), jnp.where(zi == 0, 0, n + 1)
        planes_ref[rows(z_ghost * pitch, pitch), :] = -planes_ref[rows(z_edge * pitch, pitch), :]

    def expand_zy(coarse, planes_ref, fine, z_offset, y_offset):
        half = fine.n // 2
        size = half
        pitch = coarse.pitch
        even_lane = lax.rem(lanes(size), 2) == 0

        def step(indices):
            results = []
            for k in indices:
                middle = (k + z_offset + 1) * pitch + TILE + y_offset
                low, high = {}, {}
                for dy in (-1, 0, 1):
                    here = 0.75 * planes_ref[pl.ds(middle + dy, size), :]
                    low[dy] = here + 0.25 * planes_ref[pl.ds(middle - pitch + dy, size), :]
                    high[dy] = here + 0.25 * planes_ref[pl.ds(middle + pitch + dy, size), :]
                for odd in (0, 1):
                    dy = 2 * odd - 1
                    z_even = 0.75 * low[0] + 0.25 * low[dy]
                    z_odd = 0.75 * high[0] + 0.25 * high[dy]
                    first = turn(jnp.where(even_lane, z_even, z_odd), skew(fine, k))
                    second = turn(jnp.where(even_lane, z_odd, z_even), skew(fine, k))
                    span = pl.ds((k + 1) * fine.pitch + TILE + odd, size, stride=2)
                    for colour, change in ((odd, first), (1 - odd, second)):
                        results.append((colour, span, fine.v[colour][span, :] + change))
            for colour, span, value in results:
                fine.v[colour][span, :] = value
        grouped(fine.planes, 4, step)

    barrier = pltpu.get_barrier_semaphore()
    for target in ({'x': 1 - xi}, {'y': 1 - yi}, {'z': 1 - zi}, {'z': 1 - zi, 'y': 1 - yi}):
        pl.semaphore_signal(barrier, inc=1, device_id=target, device_id_type=MESH)
    pl.semaphore_wait(barrier, 4)

    top = levels[0]
    load_chunks = 4
    chunk_rows = edge * edge // load_chunks

    def load_copy(index, which):
        span = rows(index * chunk_rows, chunk_rows)
        return pltpu.make_async_copy(
            (refs['u_in'], refs['f_in'])[which].at[span], (stage_u, stage_f)[which].at[span],
            refs['load'].at[2 * index + which])

    for index in range(load_chunks):
        for which in (0, 1):
            load_copy(index, which).start()
    even_edge = even_mask(edge)
    scale = 1.0 / float((2 * edge) ** 2)

    def pack(index, carry):
        load_copy(index, 0).wait()
        load_copy(index, 1).wait()

        per_chunk = top.planes // load_chunks

        def step(indices):
            for i in indices:
                k = index * per_chunk + i
                for stage, target, start in ((stage_u, top.v, (k + 1) * top.pitch + TILE), (stage_f, top.g, k * edge)):
                    a, b = stage[rows(2 * k * edge, edge), :], stage[rows((2 * k + 1) * edge, edge), :]
                    if stage is stage_f:
                        a, b = a * scale, b * scale
                    target[RED][rows(start, edge), :] = turn(jnp.where(even_edge, a, b), skew(top, k))
                    target[BLACK][rows(start, edge), :] = turn(jnp.where(even_edge, b, a), skew(top, k))
        grouped(per_chunk, 2, step)
        return carry
    lax.fori_loop(0, load_chunks, pack, 0)

    for index in range(len(levels) - 1):
        refs[f'mat_q{index}'][...] = restriction_matrix(levels[index].n // 2)
    refs['mat_p0'][...] = distributed_matrix(levels[1].n)
    refs['mat_p1'][...] = prolongation_matrix(levels[1].n, levels[2].n, xi * (levels[2].n // 2), None, None)
    for index in range(2, len(levels) - 1):
        fine_n = levels[index].n
        refs[f'mat_p{index}'][...] = prolongation_matrix(fine_n, fine_n // 2, 0, None, None)

    planes_dist, planes_local = refs['planes_dist'], refs['planes_local']

    def residual(level):
        half_sweep(level, RED, 'res0')
        half_sweep(level, BLACK, 'res1')

    def solve(level, sweep_count, phases, descend):
        def phase(p, carry):
            def sweep(index, inner):
                fresh = (p == 0) & (index == 0)

                @pl.when(fresh)
                def _():
                    set_zero(level.v[BLACK], (level.planes + 2) * level.pitch)
                    half_sweep(level, RED, 'zero')

                @pl.when(jnp.logical_not(fresh))
                def _():
                    half_sweep(level, RED, 'gs')
                half_sweep(level, BLACK, 'gs')
                return inner
            lax.fori_loop(0, sweep_count, sweep, 0)
            if phases == 2:
                @pl.when(p == 0)
                def _():
                    residual(level)
                    descend()
            return carry
        lax.fori_loop(0, phases, phase, 0)

    def solve_coarsest(level):
        n, planes = level.n, level.planes
        row = lax.broadcasted_iota(jnp.int32, (TILE, LANES), 0)
        lane = lanes(TILE)
        low_row, high_row = row == 0, row == n - 1
        even_row = lax.rem(row, 2) == 0
        odd_row = jnp.logical_not(even_row)

        def spread(colour, k, x):
            values = level.g[colour][rows(k * level.nb, TILE), :]
            return jnp.broadcast_to(lax.slice(values, (0, x + k), (TILE, x + k + 1)), (TILE, LANES))
        cells = [(k, x) for k in range(planes) for x in range(n)]
        scaled = [{cell: spread(colour, *cell) for cell in cells} for colour in (RED, BLACK)]

        def half(colour, own, other):
            updated = {}
            for k, x in cells:
                minus, here = -own[k, x], other[k, x]
                takes_below = even_row if (x + colour) % 2 == 0 else odd_row
                total = lax.select(takes_below, other.get((k - 1, x), minus), other.get((k + 1, x), minus)) + here
                total = total + (other.get((k, x - 1), minus) + other.get((k, x + 1), minus))
                before = lax.select(low_row, minus, pltpu.roll(here, 1, 0))
                total = total + (before + lax.select(high_row, minus, pltpu.roll(here, TILE - 1, 0)))
                updated[k, x] = (total + scaled[colour][k, x]) * SIXTH
            return updated

        def sweep(index, state):
            red, black = (dict(zip(cells, part)) for part in state)
            red = half(RED, red, black)
            black = half(BLACK, black, red)
            return tuple(tuple(part[cell] for cell in cells) for part in (red, black))
        zeros = (jnp.zeros((TILE, LANES), F32),) * len(cells)
        state = lax.fori_loop(0, COARSE_SWEEPS, sweep, (zeros, zeros))
        for colour, part in enumerate(state):
            for k in range(planes):
                plane = jnp.zeros((TILE, LANES), F32)
                for x in range(n):
                    plane = lax.select(lane == x + k, part[k * n + x], plane)
                level.v[colour][rows((k + 1) * level.pitch + TILE, TILE), :] = plane

    def solve_local(index):
        level = levels[index]
        if index == len(levels) - 1:
            solve_coarsest(level)
            return

        def descend():
            restrict_local(level, levels[index + 1], index)
            solve_local(index + 1)
            expand_x(levels[index + 1], planes_local, refs[f'mat_p{index}'][...])
            pad_local(levels[index + 1], planes_local)
            expand_zy(levels[index + 1], planes_local, level, 0, 0)
        solve(level, 2, 2, descend)

    middle, replicated = levels[1], levels[2]

    def descend_middle():
        restrict_gather(replicated)
        solve_local(2)
        expand_x(replicated, planes_local, refs['mat_p1'][...])
        pad_local(replicated, planes_local)
        expand_zy(replicated, planes_local, middle, zi * (replicated.n // 2), yi * (replicated.n // 2))
        half_sweep(middle, BLACK, 'copy')

    half_sweep(top, BLACK, 'copy')

    def sweep_pair(index, carry):
        sweeps(top, 2)

        @pl.when(lax.rem(index, 2) == 0)
        def _():
            residual(top)
            restrict_local(top, middle, 0)
            solve(middle, 2, 2, descend_middle)
            wait_all(middle, BLACK)
            expand_x(middle, planes_dist, refs['mat_p0'][...])
            pad_distributed(middle, planes_dist)
            expand_zy(middle, planes_dist, top, 0, 0)
            half_sweep(top, BLACK, 'copy')
        return carry
    lax.fori_loop(0, 2 * CYCLES, sweep_pair, 0)
    wait_all(top, BLACK)

    def store_copy(k, colour):
        return pltpu.make_async_copy(
            top.v[colour].at[rows((k + 1) * top.pitch + TILE, edge)],
            (refs['red_out'], refs['black_out'])[colour].at[rows(k * edge, edge)], refs['store'].at[2 * k + colour])

    def store_start(k, carry):
        store_copy(k, RED).start()
        store_copy(k, BLACK).start()
        return carry

    def store_wait(k, carry):
        store_copy(k, RED).wait()
        store_copy(k, BLACK).wait()
        return carry
    lax.fori_loop(0, top.planes, store_start, 0)
    lax.fori_loop(0, top.planes, store_wait, 0)


def solve_packed(initial, source, edge):
    levels = make_levels(edge)
    names = ['u_in', 'f_in', 'red_out', 'black_out']
    scratch = []

    def add(name, shape):
        names.append(name)
        scratch.append(shape)

    for index, level in enumerate(levels):
        for key, shape in level.scratch().items():
            add(f'L{index}_{key}', shape)
    add('stage_u', pltpu.VMEM((edge * edge, LANES), F32))
    add('stage_f', pltpu.VMEM((edge * edge, LANES), F32))
    add('pair_sum', pltpu.VMEM((edge * WIDTH, LANES), F32))
    for index in range(len(levels) - 1):
        add(f'mat_p{index}', pltpu.VMEM((LANES, LANES), F32))
        add(f'mat_q{index}', pltpu.VMEM((LANES, LANES), F32))
    middle, replicated = levels[1], levels[2]
    add('planes_dist', pltpu.VMEM(((middle.n + 2) * middle.pitch, LANES), F32))
    add('planes_local', pltpu.VMEM(((replicated.n + 2) * replicated.pitch, LANES), F32))
    add('pfy', pltpu.VMEM((middle.n, LANES), F32))
    add('phy', pltpu.VMEM((middle.n, LANES), F32))
    add('phc', pltpu.VMEM((TILE, LANES), F32))
    add('qs', pltpu.SemaphoreType.DMA((3,)))
    add('qr', pltpu.SemaphoreType.DMA((3,)))
    block_n = middle.n // 2
    add('gather_own', pltpu.VMEM((4 * (block_n // 4) * block_n, LANES), F32))
    add('gather_other', pltpu.VMEM((4 * (block_n // 4) * block_n, LANES), F32))
    add('gs', pltpu.SemaphoreType.DMA((3,)))
    add('gr', pltpu.SemaphoreType.DMA((3,)))
    add('ps', pltpu.SemaphoreType.DMA((4,)))
    add('pr', pltpu.SemaphoreType.DMA((4,)))
    add('load', pltpu.SemaphoreType.DMA((TILE,)))
    add('store', pltpu.SemaphoreType.DMA((edge,)))
    half = jax.ShapeDtypeStruct((edge * edge // 2, LANES), F32)
    return pl.pallas_call(
        functools.partial(kernel_body, names, edge),
        out_shape=(half, half),
        in_specs=[pl.BlockSpec(memory_space=pl.ANY)] * 2,
        out_specs=(pl.BlockSpec(memory_space=pl.ANY),) * 2,
        scratch_shapes=scratch,
        compiler_params=pltpu.CompilerParams(collective_id=0, has_side_effects=True, vmem_limit_bytes=66000000),
        name='multigrid',
    )(initial, source)


def unpack_body(red_ref, black_ref, out_ref):
    planes = red_ref.shape[0]
    first = pl.program_id(0) * planes + lax.axis_index('z') * (planes * pl.num_programs(0))
    even = lax.rem(lax.broadcasted_iota(jnp.int32, (LANES, LANES), 0) + lax.broadcasted_iota(jnp.int32, (LANES, LANES), 1), 2) == 0
    for k in range(planes):
        shift = lax.rem(2 * LANES - first - k, LANES)
        red, black = pltpu.roll(red_ref[k], shift, 1), pltpu.roll(black_ref[k], shift, 1)
        out_ref[2 * k] = jnp.where(even, red, black)
        out_ref[2 * k + 1] = jnp.where(even, black, red)


def unpack(red, black, edge):
    step = 2 * TILE
    spec = pl.BlockSpec((step, edge, LANES), lambda i: (i, 0, 0))
    return pl.pallas_call(
        unpack_body,
        grid=(edge // 2 // step,),
        out_shape=jax.ShapeDtypeStruct((edge, edge, LANES), F32),
        in_specs=[spec, spec],
        out_specs=pl.BlockSpec((2 * step, edge, LANES), lambda i: (i, 0, 0)),
        name='unpack',
    )(red.reshape(edge // 2, edge, LANES), black.reshape(edge // 2, edge, LANES))


def solution(mesh):
    grid_spec = P(('batch', 'z'), 'y', 'x')

    def local_solve(source, initial_guess):
        edge = source.shape[0]
        red, black = solve_packed(
            initial_guess.reshape(edge * edge, edge), source.reshape(edge * edge, edge), edge)
        return unpack(red, black, edge)

    return jax.shard_map(local_solve, mesh=mesh, in_specs=(grid_spec, grid_spec), out_specs=grid_spec, check_vma=False)
```
